32 devices in a mesh: leaf: 32 (over z, y, x, core).
Axes of the slice: x: 2, y: 2, z: 4, core: 2. Of those that a mesh axis runs over, the one named last changes fastest.
Arguments:
- coords: float32 [3, 262144], P(None, 'leaf'), may hold values from 0 to 1
- charges: bfloat16 [262144, 128], P('leaf'), may hold values from -6 to 6
- near_leaves: int32 [2048, 27], P('leaf'), may hold values from 0 to 191
- leaf_basis: bfloat16 [2048, 4096], P('leaf'), may hold values from -1 to 1
- leaf_transfer: bfloat16 [2048, 1024], P('leaf'), may hold values from -0.75 to 0.75
- mid_transfer: bfloat16 [256, 1024], P('leaf'), may hold values from -0.75 to 0.75
- base_transfer: bfloat16 [32, 1024], P('leaf'), may hold values from -0.75 to 0.75
- base_coupling: bfloat16 [6048, 1024], P('leaf'), may hold values from -0.01953125 to 0.01953125
- base_target: int32 [6048, 1], P('leaf'), may hold values from 0 to 31; in each aligned block of 189 rows (0 to 188, 189 to 377, ...) at most 11 rows name the same one
- base_source: int32 [6048], P('leaf'), may hold values from 0 to 31
- top_coupling: bfloat16 [256, 1024], P('leaf'), may hold values from -0.015625 to 0.015625
- top_target: int32 [256], P('leaf'), may hold values from 0 to 3
- top_source: int32 [256], P('leaf'), may hold values from 0 to 3
Outputs:
- potential: bfloat16 [262144, 128], P('leaf')
The draws below stay inside these ranges and needn't reach their ends.
Inputs may be any that keep to these rules, and one draw needn't show every extreme that they name: `near_leaves`: entry j of leaf l names leaf 64 * (l // 64 - 1) + j: a leaf of the device before in Morton order, of the row's own device, or of the device after; repeats may occur. `base_target`: among the 189 blocks of one device no base cluster is the target more than 11 times; that count is reached.
All inputs are finite; a program needn't handle non-finite values.
Results may differ from the reference program's by a relative error of at most 0.01.
Values may be sent and summed in bfloat16 or wider, within the bound.
A program may use at most 128 MiB of HBM per device.

```python
import math
import jax
import jax.numpy as jnp
import numpy as np
from jax import lax

K = 32
RHS = 128
M = 128
NNEAR = 27
NB = 189
TOPB_DEV = 8
LEAF_DEV = 64
BASE_DEV = 1
LEAVES = 2048
NPTS = 262144
MIDS = 256
NBASE = 32
NTOP = 4
BLK_DEV = 189
NBLK = 6048
NTBLK = 256
CAPC = 11
N_LEAF = 32


def set_ends(drawn, stream_key, smallest, top_value):
    shape = drawn.shape
    spot = [jax.random.randint(jax.random.fold_in(stream_key, axis), (), 0, shape[axis]) for axis in range(len(shape))]
    drawn = drawn.at[tuple(spot)].set(smallest)
    longest = shape.index(max(shape))
    spot[longest] = (spot[longest] + 1) % shape[longest]
    return drawn.at[tuple(spot)].set(top_value)


def shard_levels(rng, dims, pieces, smallest, high):
    loudness, own = 1.0, jax.random.fold_in(rng, 6)
    for position, blocks in pieces:
        draws = jnp.exp(jax.random.uniform(jax.random.fold_in(own, position), (blocks,), jnp.float32, smallest / len(pieces), high / len(pieces)))
        loudness = loudness * jnp.repeat(draws, dims[position] // blocks).reshape([-1 if axis == position else 1 for axis in range(len(dims))])
    return loudness


def shared_out(rng, own, number, rows, amount, top, bound, slope):
    ranking = jax.random.permutation(rng, amount)
    heavy_load, ordinary = shares(amount, rows * top, bound, slope, True), shares(amount, rows * top, bound, slope, False)
    places = jnp.arange(amount)

    def named(lengths, offset_by):
        used = int((lengths > 0).sum())
        fixed = max(1, used // 4)
        passed = fixed + (places - fixed + offset_by * (used - fixed)) % max(1, amount - fixed)
        return jnp.zeros((amount,), jnp.int32).at[ranking[jnp.where(places < fixed, places, passed)]].set(jnp.asarray(lengths, jnp.int32))

    lengths = jnp.where(number % 4 == 0, named(heavy_load, number // 4), named(ordinary, number - number // 4 - 1))
    mixed = jax.random.permutation(jax.random.fold_in(own, 3), amount)
    source_of, taker = mixed[0:amount // 2 * 2:2], mixed[1:amount // 2 * 2:2]
    margin = jnp.minimum(lengths[source_of] - 1, bound - lengths[taker]) // 2
    margin = jnp.where((source_of == ranking[0]) | (taker == ranking[0]) | (lengths[taker] == 0), 0, jnp.maximum(margin, 0))
    passed = jax.random.randint(jax.random.fold_in(own, 4), (amount // 2,), 0, 1 << 20) % (margin + 1)
    lengths = lengths.at[source_of].add(-passed).at[taker].add(passed)
    labels = jnp.searchsorted(jnp.cumsum(lengths), jnp.arange(rows * top), side="right").astype(jnp.int32)
    listing = labels.reshape(top, rows).T
    listing = listing[jax.random.permutation(jax.random.fold_in(own, 1), rows)]
    offset_by = jax.random.randint(jax.random.fold_in(own, 2), (rows, 1), 0, top)
    return jnp.take_along_axis(listing, (jnp.arange(top)[None, :] + offset_by) % top, axis=1)


def shares(count, total, bound, lean, full):
    weights = [(1 << 20) // math.isqrt(grade ** lean) + 1 for grade in range(1, count + 1)]
    largest = bound if full else min(bound, max(-(-total // count), total * weights[0] // sum(weights)))
    least = 1 if total - largest >= count - 1 else 0
    counts, spare = [largest] + [least] * (count - 1), total - largest - least * (count - 1)
    while spare > 0:
        movable = [i for i in range(1, count) if counts[i] < largest] or [i for i in range(1, count) if counts[i] < bound]
        whole, remaining = sum([weights[i] for i in movable]), spare
        for i in movable:
            more = min(bound - counts[i], max(1, remaining * weights[i] // whole), spare)
            counts[i] = counts[i] + more
            spare = spare - more
    return np.array(counts)


def centred(key, dims, spread, bound, pieces=(), kind=jnp.bfloat16):
    result = spread * jax.random.normal(key, dims, jnp.float32)
    if pieces:
        result = result * shard_levels(key, dims, pieces, -0.22, 0.18)
    return jnp.clip(result, -bound, bound).astype(kind)


def setup_inputs(seed: int = 0) -> dict:
    arg_keys = jax.random.split(jax.random.key(seed), 14)
    coords = jnp.clip(1.0 * jax.random.uniform(arg_keys[0], (3, NPTS), jnp.float32) ** shard_levels(arg_keys[0], (3, NPTS), ((1, 32),), -0.2, 0.2), 0.0, 1.0)
    charges = centred(arg_keys[1], (NPTS, RHS), 1.0, 6.0, ((0, 32),))
    near_leaves = set_ends(jax.random.randint(arg_keys[2], (LEAVES, NNEAR), 0, 3 * LEAF_DEV), jax.random.fold_in(arg_keys[2], 1), 0, (3 * LEAF_DEV) - 1).astype(jnp.int32)
    leaf_basis = centred(arg_keys[3], (LEAVES, K * M), K ** -0.5, 1.0, ((0, 32),))
    leaf_transfer = centred(arg_keys[4], (LEAVES, K * K), (2 * K) ** -0.5, 0.75, ((0, 32),))
    mid_transfer = centred(arg_keys[5], (MIDS, K * K), (2 * K) ** -0.5, 0.75, ((0, 32),))
    base_transfer = centred(arg_keys[6], (NBASE, K * K), (2 * K) ** -0.5, 0.75, ((0, 32),))
    base_coupling = centred(arg_keys[7], (NBLK, K * K), (16 * K * NB) ** -0.5, 0.01953125, ((0, 32),))
    base_target_keys = jax.random.split(jax.random.fold_in(arg_keys[8], 1), NBLK // BLK_DEV)
    base_target_turns = jax.random.permutation(jax.random.fold_in(arg_keys[8], 3), NBLK // BLK_DEV)
    base_target = jax.vmap(lambda own, number: shared_out(jax.random.fold_in(arg_keys[8], 2), own, number, BLK_DEV, NBASE, 1, CAPC, 1))(base_target_keys, base_target_turns).reshape((NBLK, 1))
    base_source = set_ends(jax.random.randint(arg_keys[9], (NBLK,), 0, NBASE), jax.random.fold_in(arg_keys[9], 1), 0, NBASE - 1).astype(jnp.int32)
    top_coupling = centred(arg_keys[10], (NTBLK, K * K), (512 * K * TOPB_DEV // BASE_DEV) ** -0.5, 0.015625, ((0, 32),))
    top_target = set_ends(jax.random.randint(arg_keys[11], (NTBLK,), 0, NTOP), jax.random.fold_in(arg_keys[11], 1), 0, NTOP - 1).astype(jnp.int32)
    top_source = set_ends(jax.random.randint(arg_keys[12], (NTBLK,), 0, NTOP), jax.random.fold_in(arg_keys[12], 1), 0, NTOP - 1).astype(jnp.int32)
    return {"coords": coords, "charges": charges, "near_leaves": near_leaves, "leaf_basis": leaf_basis, "leaf_transfer": leaf_transfer, "mid_transfer": mid_transfer, "base_transfer": base_transfer, "base_coupling": base_coupling, "base_target": base_target, "base_source": base_source, "top_coupling": top_coupling, "top_target": top_target, "top_source": top_source}


delta_sq = 0.0025

def rounded_values(values):
    return lax.optimization_barrier(values.astype(jnp.bfloat16))

def near_block(points, pool_points, pool_charges, columns):
    near_scale = 1.0 / math.sqrt(columns.shape[1] * points.shape[2])

    def near_step(running, column):
        other_points = jnp.take(pool_points, column, axis=1)
        other_charges = jnp.take(pool_charges, column, axis=0)
        squares = lax.optimization_barrier(jnp.sum((points[:, :, :, None] - other_points[:, :, None, :]) ** 2, axis=0))
        kernel = rounded_values(near_scale / jnp.sqrt(squares + delta_sq))
        update = jnp.einsum('lab,lbr->lar', kernel.astype(jnp.float32), other_charges.astype(jnp.float32))
        return (running + update, None)
    initial = jnp.zeros((points.shape[1], points.shape[2], pool_charges.shape[2]), jnp.float32)
    running, unused = lax.scan(near_step, initial, columns.T)
    return running

def reference(coords, charges, near_leaves, leaf_basis, leaf_transfer, mid_transfer, base_transfer, base_coupling, base_target, base_source, top_coupling, top_target, top_source):
    single_precision = jnp.float32
    charge_row_block = charges.reshape(LEAVES, M, RHS)
    basis_matrix = leaf_basis.reshape(LEAVES, K, M)
    leaf_coefficients = rounded_values(jnp.einsum('xpt,xtu->xpu', basis_matrix.astype(single_precision), charge_row_block.astype(single_precision)))
    mid_coeffs = rounded_values(jnp.einsum('mckp,mckr->mpr', leaf_transfer.reshape(MIDS, 8, K, K).astype(single_precision), leaf_coefficients.reshape(MIDS, 8, K, RHS).astype(single_precision)))
    base_coeffs = rounded_values(jnp.einsum('mckp,mckr->mpr', mid_transfer.reshape(NBASE, 8, K, K).astype(single_precision), mid_coeffs.reshape(NBASE, 8, K, RHS).astype(single_precision)))
    base_lift = base_transfer.reshape(NBASE, K, K)
    lifted = rounded_values(jnp.einsum('bkp,bkr->bpr', base_lift.astype(single_precision), base_coeffs.astype(single_precision)))
    top_coeffs = rounded_values(lax.optimization_barrier(jnp.sum(lifted.reshape(NTOP, 8, K, RHS).astype(single_precision), axis=1)))

    def add_portion(running, portion):
        blocks, targets, sources = portion
        products = jnp.einsum('bts,bsr->btr', blocks.reshape(-1, K, K).astype(single_precision), jnp.take(base_coeffs, sources, axis=0).astype(single_precision))
        return (running + jax.ops.segment_sum(products, targets, num_segments=NBASE), None)
    portions = (base_coupling.reshape(N_LEAF, BLK_DEV, K * K), base_target.reshape(N_LEAF, BLK_DEV), base_source.reshape(N_LEAF, BLK_DEV))
    coupled, unused = lax.scan(add_portion, jnp.zeros((NBASE, K, RHS), single_precision), portions)
    top_products = jnp.einsum('bts,bsr->btr', top_coupling.reshape(NTBLK, K, K).astype(single_precision), jnp.take(top_coeffs, top_source, axis=0).astype(single_precision))
    top_field = rounded_values(jax.ops.segment_sum(top_products, top_target, num_segments=NTOP))
    base_field = rounded_values(coupled + jnp.einsum('bkp,bpr->bkr', base_lift.astype(single_precision), jnp.repeat(top_field, 8, axis=0).astype(single_precision)))
    mid_field = rounded_values(jnp.einsum('mkp,mpr->mkr', mid_transfer.reshape(MIDS, K, K).astype(single_precision), jnp.repeat(base_field, 8, axis=0).astype(single_precision)))
    leaf_potential = rounded_values(jnp.einsum('lkp,lpr->lkr', leaf_transfer.reshape(LEAVES, K, K).astype(single_precision), jnp.repeat(mid_field, 8, axis=0).astype(single_precision)))
    all_points = coords.reshape(3, LEAVES, M)
    padded_points = jnp.pad(all_points, ((0, 0), (LEAF_DEV, LEAF_DEV), (0, 0)))
    padded_charges = jnp.pad(charge_row_block, ((LEAF_DEV, LEAF_DEV), (0, 0), (0, 0)))
    device_ids = jnp.arange(N_LEAF, dtype=jnp.int32)

    def device_block(portion):
        device, columns, local_expansion_basis, local_potential = portion
        first = (device * LEAF_DEV).astype(jnp.int32)
        points = lax.dynamic_slice_in_dim(all_points, first, LEAF_DEV, 1)
        pool_points = lax.dynamic_slice_in_dim(padded_points, first, 3 * LEAF_DEV, 1)
        pool_charges = lax.dynamic_slice_in_dim(padded_charges, first, 3 * LEAF_DEV, 0)
        near_field = near_block(points, pool_points, pool_charges, columns)
        distant_field = jnp.einsum('cbz,cbw->czw', local_expansion_basis.astype(single_precision), local_potential.astype(single_precision))
        return (near_field + distant_field).astype(jnp.bfloat16)
    inputs = (device_ids, near_leaves.reshape(N_LEAF, LEAF_DEV, NNEAR), basis_matrix.reshape(N_LEAF, LEAF_DEV, K, M), leaf_potential.reshape(N_LEAF, LEAF_DEV, K, RHS))
    potential = lax.map(device_block, inputs)
    return potential.reshape(NPTS, RHS)
```

```python
import functools
import math

import jax
import jax.numpy as jnp
from jax import lax
from jax.experimental import pallas as pl
from jax.experimental.pallas import tpu as pltpu
from jax.sharding import PartitionSpec as P

K = 32
RHS = 128
M = 128
FEATURES = 32
DELTA_SQ = 0.0025
CHUNKS = 16
EACH = 2
WIDTH = 1024

F32 = jnp.float32
BF16 = jnp.bfloat16
MESH = pl.DeviceIdType.MESH
VMEM = pl.BlockSpec(memory_space=pltpu.VMEM)
SMEM = pl.BlockSpec(memory_space=pltpu.SMEM)
ANY = pl.BlockSpec(memory_space=pl.ANY)


def dot(a, b):
    return jnp.dot(a, b, preferred_element_type=F32)


def dot_ta(a, b):
    return lax.dot_general(a, b, (((0,), (0,)), ((), ())), preferred_element_type=F32)


def rows(index, size):
    return pl.ds(pl.multiple_of(index * size, size), size)


def pieces(x):
    high = x.astype(BF16).astype(F32)
    rest = x - high
    middle = rest.astype(BF16).astype(F32)
    return high, middle, (rest - middle).astype(BF16).astype(F32)


def write_features(rows_ref, first, width, parts):
    at = 0
    for part in parts:
        rows_ref[at : at + part.shape[0], pl.ds(first, width)] = part
        at += part.shape[0]


def groups_of(named):
    return [range(j, min(j + 2, named)) for j in range(0, named, 2)]


def levels_of(devices):
    half = devices // 2
    low = 2 ** (int(math.log2(half // 4)) // 2)
    levels, stride = [], 1
    for size in (low, half // 4 // low, 4):
        levels.append((stride, size))
        stride *= size
    return levels


def exchange_kernel(
    devices, leaves, named, blocks, top_blocks, step, scale,
    near_ref, source_ref, top_source_ref,
    coords_ref, charges_ref,
    top_target_ref, target_ref, basis_ref, leaf_t_ref, mid_t_ref, base_t_ref, blocks_ref, top_blocks_ref,
    kernels_ref, before_ref, after_ref, fields_ref,
    points, own, features, targets, staged, made, coeffs, gathered,
    products, partial, core_got, top_coeffs, *rest,
):
    levels = levels_of(devices)
    currents, receives = rest[: len(levels)], rest[len(levels) : 2 * len(levels)]
    (local_sem, made_sem, point_send, point_recv, up_send, down_send, near_recv,
     gather_send, gather_recv, reduce_send, reduce_recv) = rest[2 * len(levels) :]
    count = leaves * M
    part = count // CHUNKS
    half = devices // 2
    me = lax.axis_index("leaf")
    core, place = me % 2, me // 2
    has_before, has_after = me > 0, me < devices - 1
    twin = place * 2 + (1 - core)

    own_copy = pltpu.make_async_copy(charges_ref, own, local_sem.at[0])
    own_points = pltpu.make_async_copy(coords_ref, points.at[1], local_sem.at[1])
    own_points.start()
    own_copy.start()

    def digit(stride, size):
        return (place // stride) % size

    def peer(stride, size, turn):
        mine = digit(stride, size)
        other = (mine + turn) % size
        return other, (place + (other - mine) * stride) * 2 + core

    barrier = pltpu.get_barrier_semaphore()
    met = 1
    pl.semaphore_signal(barrier, inc=1, device_id=(twin,), device_id_type=MESH)
    for stride, size in levels:
        for turn in range(1, size):
            met += 1
            pl.semaphore_signal(
                barrier, inc=1, device_id=(peer(stride, size, turn)[1],), device_id_type=MESH
            )

    @pl.when(has_before)
    def _():
        pl.semaphore_signal(barrier, inc=1, device_id=(me - 1,), device_id_type=MESH)

    @pl.when(has_after)
    def _():
        pl.semaphore_signal(barrier, inc=1, device_id=(me + 1,), device_id_type=MESH)

    pl.semaphore_wait(
        barrier, met + jnp.where(has_before, 1, 0) + jnp.where(has_after, 1, 0)
    )

    def remote(src, dst, send, recv, device):
        return pltpu.make_async_remote_copy(
            src_ref=src, dst_ref=dst, send_sem=send, recv_sem=recv,
            device_id=(device,), device_id_type=MESH,
        )

    def points_up():
        return remote(coords_ref, points.at[0], point_send.at[0], point_recv.at[0], me + 1)

    def points_down():
        return remote(coords_ref, points.at[2], point_send.at[1], point_recv.at[1], me - 1)

    def chunk_up(c):
        return remote(
            charges_ref.at[rows(c, part), :], before_ref.at[rows(c, part), :],
            up_send.at[c], near_recv.at[0], me + 1,
        )

    def chunk_down(c):
        return remote(
            charges_ref.at[rows(c, part), :], after_ref.at[rows(c, part), :],
            down_send.at[c], near_recv.at[1], me - 1,
        )

    def send_chunk(c):
        @pl.when(has_after)
        def _():
            chunk_up(c).start()

        @pl.when(has_before)
        def _():
            chunk_down(c).start()

    @pl.when(has_after)
    def _():
        points_up().start()

    @pl.when(has_before)
    def _():
        points_down().start()

    @pl.when(jnp.logical_not(has_before))
    def _():
        points[0] = jnp.zeros((3, count), F32)

    @pl.when(jnp.logical_not(has_after))
    def _():
        points[2] = jnp.zeros((3, count), F32)

    send_chunk(0)
    send_chunk(1)

    own_copy.wait()

    def up_group(i, carry):
        for j in range(8):
            leaf = i * 8 + j
            coeffs[rows(leaf, K), :] = dot(
                basis_ref[rows(leaf, K), :], own[rows(leaf, M), :]
            ).astype(BF16)
        return carry

    lax.fori_loop(0, leaves // 8, up_group, 0)
    mids = []
    for m in range(leaves // 8):
        area = slice(m * 8 * K, (m + 1) * 8 * K)
        mids.append(dot_ta(leaf_t_ref[area, :], coeffs[area, :]).astype(BF16))
    base = dot_ta(mid_t_ref[...], jnp.concatenate(mids, axis=0)).astype(BF16)
    spot = core * half + place
    gathered[spot] = jnp.concatenate(
        [base, dot_ta(base_t_ref[...], base).astype(BF16)], axis=0
    )

    def featured(which):
        def chunk(i, carry):
            first = pl.multiple_of(i * WIDTH, WIDTH)
            x = (points[which, :, pl.ds(first, WIDTH)] - 0.5) * scale
            h, m, l = pieces(x)
            norm = x[0:1] * x[0:1] + x[1:2] * x[1:2] + x[2:3] * x[2:3]
            ones = jnp.ones((3, WIDTH), F32)
            zeros = jnp.zeros((FEATURES - 24, WIDTH), F32)
            if which == 1:
                n = pieces(norm + DELTA_SQ * scale * scale)
                write_features(targets, first, WIDTH, [h, h, m, h, l, m, *n, ones, zeros])
            n = pieces(norm)
            h, m, l = -2.0 * h, -2.0 * m, -2.0 * l
            write_features(staged, 0, WIDTH, [h, m, h, l, h, m, ones, *n, zeros])
            for k in range(WIDTH // M):
                features[which * leaves + i * (WIDTH // M) + k] = staged[
                    :, k * M : (k + 1) * M
                ].astype(BF16)
            return carry

        lax.fori_loop(0, count // WIDTH, chunk, 0)

    def gather_copies(level):
        if level == len(levels):
            where = rows(core, half)
            return [remote(
                gathered.at[where], gathered.at[where],
                gather_send.at[level, 0], gather_recv.at[level, 0], twin,
            )]
        stride, size = levels[level]
        copies = []
        for turn in range(1, size):
            where = rows((core * half + place) // stride, stride)
            copies.append(remote(
                gathered.at[where], gathered.at[where],
                gather_send.at[level, turn - 1], gather_recv.at[level, turn - 1],
                peer(stride, size, turn)[1],
            ))
        return copies

    def reduce_copies(level):
        if level == len(levels):
            return [remote(
                partial.at[rows(1 - core, half * 2 * K), :], core_got,
                reduce_send.at[level, 0], reduce_recv.at[level, 0], twin,
            )]
        stride, size = levels[level]
        copies = []
        for turn in range(1, size):
            other, device = peer(stride, size, turn)
            copies.append(remote(
                currents[level].at[rows(other, stride * 2 * K), :], receives[level].at[turn - 1],
                reduce_send.at[level, turn - 1], reduce_recv.at[level, turn - 1], device,
            ))
        return copies

    def start(copies):
        for copy in copies:
            copy.start()

    def arrived(copies):
        for copy in copies:
            copy.wait_recv()

    def sent(copies):
        for copy in copies:
            copy.wait_send()

    def spot_of(device):
        return (device % 2) * half + device // 2

    def couple():
        for t in range(devices // 8):
            total = jnp.zeros((K, RHS), F32)
            for j in range(8):
                total = total + gathered[spot_of(t * 8 + j), K:, :].astype(F32)
            top_coeffs[t] = total.astype(BF16)

        def group(i, carry):
            for j in range(step):
                b = i * step + j
                source = source_ref[b]
                where = (source & 1) * half + (source >> 1)
                products[rows(b, K), :] = dot(
                    blocks_ref[rows(b, K), :], gathered[where, :K, :]
                )
            return carry

        lax.fori_loop(0, blocks // step, group, 0)
        named_spot = target_ref[...]
        named_spot = (named_spot & 1) * half + (named_spot >> 1)
        ids = lax.broadcasted_iota(jnp.int32, (devices, blocks), 0)
        chosen = jnp.where(ids == named_spot, 1.0, 0.0).astype(BF16)

        def scatter(k, carry):
            terms = products[pl.ds(k, blocks, stride=K), :].astype(BF16)
            partial[pl.ds(k, devices, stride=2 * K), :] = dot(chosen, terms)
            return carry

        lax.fori_loop(0, K, scatter, 0)
        terms = [
            dot(top_blocks_ref[b * K : (b + 1) * K, :], top_coeffs[top_source_ref[b]])
            for b in range(top_blocks)
        ]
        for t in range(devices // 8):
            total = jnp.zeros((K, RHS), F32)
            for b in range(top_blocks):
                total = total + jnp.where(top_target_ref[b : b + 1, :] == t, 1.0, 0.0) * terms[b]
            for j in range(8):
                first = spot_of(t * 8 + j) * 2 * K + K
                partial[first : first + K, :] = total

    def reduced_core():
        mine = partial[rows(core, half * 2 * K), :]
        currents[-1][...] = (mine + core_got[...]).astype(BF16)

    def reduced(level):
        stride, size = levels[level]
        total = currents[level][rows(digit(stride, size), stride * 2 * K), :].astype(F32)
        for turn in range(1, size):
            total = total + receives[level][turn - 1].astype(F32)
        return total

    own_points.wait()
    featured(1)
    start(gather_copies(0))
    send_chunk(2)

    @pl.when(has_before)
    def _():
        points_up().wait_recv()

    @pl.when(has_after)
    def _():
        points_down().wait_recv()

    featured(0)
    featured(2)
    send_chunk(3)

    stages = []
    for level in range(len(levels)):
        def gather(level=level):
            arrived(gather_copies(level))
            start(gather_copies(level + 1))
        stages.append((2 * level + 1, gather))
    at = 2 * len(levels) + 1

    def coupled():
        arrived(gather_copies(len(levels)))
        couple()

    stages.append((at, coupled))
    stages.append((at + 1, lambda: start(reduce_copies(len(levels)))))

    def core_reduced():
        arrived(reduce_copies(len(levels)))
        reduced_core()

    stages.append((at + 3, core_reduced))
    at += 4
    for level in range(len(levels) - 1, -1, -1):
        stages.append((at, lambda level=level: start(reduce_copies(level))))
        if level:
            def reduce(level=level):
                arrived(reduce_copies(level))
                currents[level - 1][...] = reduced(level).astype(BF16)
            stages.append((at + 3, reduce))
        at += 4

    def made_copy(i, slot):
        return pltpu.make_async_copy(
            made.at[slot], kernels_ref.at[pl.ds(i * EACH, EACH)], made_sem.at[slot]
        )

    steps = leaves // EACH

    def make(i, carry):
        for when, stage in stages:
            pl.when(i == when)(stage)

        @pl.when((i % 2 == 0) & (i < 2 * (CHUNKS - 4)))
        def _():
            send_chunk(4 + i // 2)

        slot = i % 2

        @pl.when(i >= 2)
        def _():
            made_copy(i - 2, slot).wait()

        for k in range(EACH):
            leaf = i * EACH + k
            mine = targets[:, rows(leaf, M)].T.astype(BF16)
            for group in groups_of(named):
                theirs = jnp.concatenate(
                    [features[near_ref[leaf, j]] for j in group], axis=1
                )
                squares = dot(mine, theirs)
                made[slot, k, :, group[0] * M : (group[-1] + 1) * M] = lax.rsqrt(
                    squares.astype(BF16)
                )
        made_copy(i, slot).start()
        return carry

    lax.fori_loop(0, steps, make, 0)
    arrived(reduce_copies(0))
    total = reduced(0)
    base = (total[:K] + dot(base_t_ref[...], total[K:].astype(BF16))).astype(BF16)
    mid = dot(mid_t_ref[...], base).astype(BF16)
    for m in range(leaves // 8):
        area = slice(m * 8 * K, (m + 1) * 8 * K)
        fields_ref[area, :] = dot(leaf_t_ref[area, :], mid[m * K : (m + 1) * K, :]).astype(BF16)

    made_copy(steps - 2, steps % 2).wait()
    made_copy(steps - 1, (steps - 1) % 2).wait()

    def zero(out_ref, sem):
        own[0:part, :] = jnp.zeros((part, RHS), BF16)

        def each(c, carry):
            copy = pltpu.make_async_copy(own.at[pl.ds(0, part), :], out_ref.at[rows(c, part), :], sem)
            copy.start()
            copy.wait()
            return carry

        lax.fori_loop(0, CHUNKS, each, 0)

    for level in range(len(levels) + 1):
        sent(gather_copies(level))
        sent(reduce_copies(level))

    def drain_up(c, carry):
        chunk_up(c).wait_send()
        return carry

    def drain_down(c, carry):
        chunk_down(c).wait_send()
        return carry

    @pl.when(has_after)
    def _():
        points_up().wait_send()
        lax.fori_loop(0, CHUNKS, drain_up, 0)
        remote(charges_ref, after_ref, up_send.at[0], near_recv.at[1], me + 1).wait_recv()

    @pl.when(has_before)
    def _():
        points_down().wait_send()
        lax.fori_loop(0, CHUNKS, drain_down, 0)
        remote(charges_ref, before_ref, up_send.at[0], near_recv.at[0], me - 1).wait_recv()

    @pl.when(jnp.logical_not(has_before))
    def _():
        zero(before_ref, local_sem.at[0])

    @pl.when(jnp.logical_not(has_after))
    def _():
        zero(after_ref, local_sem.at[0])


def use_kernel(
    leaves, named,
    near_ref, kernel_ref, before_ref, own_ref, after_ref, fields_ref, basis_ref, out_ref,
    pool, sems,
):
    points = leaves * M

    @pl.when(pl.program_id(0) == 0)
    def _():
        copies = [
            pltpu.make_async_copy(ref, pool.at[pl.ds(i * points, points), :], sems.at[i])
            for i, ref in enumerate((before_ref, own_ref, after_ref))
        ]
        for copy in copies:
            copy.start()
        for copy in copies:
            copy.wait()

    for k in range(kernel_ref.shape[0]):
        leaf = pl.program_id(0) * kernel_ref.shape[0] + k
        total = dot_ta(basis_ref[rows(leaf, K), :], fields_ref[rows(leaf, K), :])
        for group in groups_of(named):
            theirs = jnp.concatenate([pool[rows(near_ref[leaf, j], M), :] for j in group], axis=0)
            total = total + dot(kernel_ref[k, :, group[0] * M : (group[-1] + 1) * M], theirs)
        out_ref[k * M : (k + 1) * M, :] = total.astype(BF16)


def per_device(
    coords,
    charges,
    near_leaves,
    leaf_basis,
    leaf_transfer,
    mid_transfer,
    base_transfer,
    base_coupling,
    base_target,
    base_source,
    top_coupling,
    top_target,
    top_source,
):
    leaves, named = near_leaves.shape
    devices = lax.axis_size("leaf")
    blocks, top_blocks = base_coupling.shape[0], top_coupling.shape[0]
    scale = math.sqrt(named * M)
    count = leaves * M
    half = devices // 2
    levels = levels_of(devices)
    widest = max(size for _, size in levels)
    basis = leaf_basis.reshape(-1, M)
    leaf_t = leaf_transfer.reshape(-1, K)
    mid_t = mid_transfer.reshape(-1, K)
    base_t = base_transfer.reshape(-1, K)

    step = max(s for s in range(1, 33) if blocks % s == 0)
    kernels, before, after, fields = pl.pallas_call(
        functools.partial(
            exchange_kernel, devices, leaves, named, blocks, top_blocks, step, scale
        ),
        out_shape=[
            jax.ShapeDtypeStruct((leaves, M, named * M), BF16),
            jax.ShapeDtypeStruct((count, RHS), BF16),
            jax.ShapeDtypeStruct((count, RHS), BF16),
            jax.ShapeDtypeStruct((leaves * K, RHS), BF16),
        ],
        in_specs=[SMEM] * 3 + [ANY] * 2 + [VMEM] * 8,
        out_specs=[ANY] * 3 + [VMEM],
        scratch_shapes=[
            pltpu.VMEM((3, 3, count), F32),
            pltpu.VMEM((count, RHS), BF16),
            pltpu.VMEM((3 * leaves, FEATURES, M), BF16),
            pltpu.VMEM((FEATURES, count), F32),
            pltpu.VMEM((FEATURES, WIDTH), F32),
            pltpu.VMEM((2, EACH, M, named * M), BF16),
            pltpu.VMEM((leaves * K, RHS), BF16),
            pltpu.VMEM((devices, 2 * K, RHS), BF16),
            pltpu.VMEM((blocks * K, RHS), F32),
            pltpu.VMEM((devices * 2 * K, RHS), F32),
            pltpu.VMEM((half * 2 * K, RHS), F32),
            pltpu.VMEM((devices // 8, K, RHS), BF16),
        ]
        + [pltpu.VMEM((stride * size * 2 * K, RHS), BF16) for stride, size in levels]
        + [pltpu.VMEM((size - 1, stride * 2 * K, RHS), BF16) for stride, size in levels]
        + [
            pltpu.SemaphoreType.DMA((2,)),
            pltpu.SemaphoreType.DMA((2,)),
            pltpu.SemaphoreType.DMA((2,)),
            pltpu.SemaphoreType.DMA((2,)),
            pltpu.SemaphoreType.DMA((CHUNKS,)),
            pltpu.SemaphoreType.DMA((CHUNKS,)),
            pltpu.SemaphoreType.DMA((2,)),
        ]
        + [pltpu.SemaphoreType.DMA((len(levels) + 1, widest - 1))] * 4,
        compiler_params=pltpu.CompilerParams(
            vmem_limit_bytes=60 * 1024 * 1024, collective_id=0, has_side_effects=True
        ),
        cost_estimate=pl.CostEstimate(
            flops=16_000_000_000, bytes_accessed=70_000_000, transcendentals=28_000_000
        ),
        name="exchange",
    )(
        near_leaves, base_source, top_source, coords, charges,
        top_target.reshape(-1, 1), base_target.reshape(1, blocks), basis, leaf_t, mid_t, base_t,
        base_coupling.reshape(-1, K), top_coupling.reshape(-1, K),
    )
    each = 4
    return pl.pallas_call(
        functools.partial(use_kernel, leaves, named),
        grid=(leaves // each,),
        out_shape=jax.ShapeDtypeStruct((count, RHS), BF16),
        in_specs=[SMEM, pl.BlockSpec((each, M, named * M), lambda i: (i, 0, 0)), ANY, ANY, ANY]
        + [VMEM] * 2,
        out_specs=pl.BlockSpec((each * M, RHS), lambda i: (i, 0)),
        scratch_shapes=[
            pltpu.VMEM((3 * count, RHS), BF16),
            pltpu.SemaphoreType.DMA((3,)),
        ],
        compiler_params=pltpu.CompilerParams(vmem_limit_bytes=48 * 1024 * 1024),
        cost_estimate=pl.CostEstimate(
            flops=8_000_000_000, bytes_accessed=66_000_000, transcendentals=0
        ),
        name="use",
    )(near_leaves, kernels, before, charges, after, fields, basis)


def solution(mesh):
    split, flat = P("leaf", None), P("leaf")
    in_specs = (P(None, "leaf"),) + (split,) * 8 + (flat, split, flat, flat)
    return jax.shard_map(
        per_device, mesh=mesh, in_specs=in_specs, out_specs=split, check_vma=False
    )
```

```python
import functools
import math

import jax
import jax.numpy as jnp
from jax import lax
from jax.experimental import pallas as pl
from jax.experimental.pallas import tpu as pltpu
from jax.sharding import PartitionSpec as P

K = 32
RHS = 128
M = 128
FEATURES = 32
DELTA_SQ = 0.0025
CHUNKS = 16
EACH = 2
WIDTH = 2048
LANES = 128
FOLD = LANES // K

F32 = jnp.float32
BF16 = jnp.bfloat16
MESH = pl.DeviceIdType.MESH
VMEM = pl.BlockSpec(memory_space=pltpu.VMEM)
SMEM = pl.BlockSpec(memory_space=pltpu.SMEM)
ANY = pl.BlockSpec(memory_space=pl.ANY)


def dot(a, b):
    return jnp.dot(a, b, preferred_element_type=F32)


def dot_ta(a, b):
    return lax.dot_general(a, b, (((0,), (0,)), ((), ())), preferred_element_type=F32)


def rows(index, size):
    return pl.ds(pl.multiple_of(index * size, size), size)


def halves(x):
    high = x.astype(BF16).astype(F32)
    return high, (x - high).astype(BF16).astype(F32)


def spread(dst, src, count):
    lane = lax.broadcasted_iota(jnp.int32, (1, LANES), 1) // K
    masks = [jnp.where(lane == f, 1.0, 0.0) for f in range(FOLD)]
    for tile in range(K // FOLD):
        slab = src[:, tile * LANES : (tile + 1) * LANES].astype(F32)
        for f in range(FOLD):
            dst[pl.ds(tile * FOLD + f, count, stride=K), :] = slab * masks[f]


def folded(x):
    return sum(x[f * K : (f + 1) * K, :] for f in range(1, FOLD)) + x[:K, :]


def tiled(x):
    return jnp.concatenate([x] * FOLD, axis=0)


def pieces(x):
    high = x.astype(BF16).astype(F32)
    rest = x - high
    middle = rest.astype(BF16).astype(F32)
    return high, middle, (rest - middle).astype(BF16).astype(F32)


def write_features(rows_ref, first, width, parts):
    at = 0
    for part in parts:
        rows_ref[at : at + part.shape[0], pl.ds(first, width)] = part
        at += part.shape[0]


def groups_of(named):
    return [range(j, min(j + 2, named)) for j in range(0, named, 2)]


def levels_of(devices):
    half = devices // 2
    low = 2 ** (int(math.log2(half // 4)) // 2)
    levels, stride = [], 1
    for size in (low, half // 4 // low, 4):
        levels.append((stride, size))
        stride *= size
    return levels


def exchange_kernel(
    devices, leaves, named, blocks, top_blocks, step, scale,
    source_ref, top_target_ref, top_source_ref,
    near_ref, coords_ref, charges_ref,
    target_ref, basis_ref, leaf_t_ref, mid_t_ref, base_t_ref, blocks_ref, top_blocks_ref,
    kernels_ref, before_ref, after_ref, fields_ref, basis_out,
    named_leaves, points, own, features, targets, staged, made, coeffs, gathered,
    zeros_part, basis, leaf_t, mid_t, base_t, top_t, wide, products, partial, core_got,
    top_coeffs, *rest,
):
    levels = levels_of(devices)
    currents, receives = rest[: len(levels)], rest[len(levels) : 2 * len(levels)]
    (local_sem, made_sem, point_send, point_recv, up_send, down_send, near_recv,
     gather_send, gather_recv, reduce_send, reduce_recv) = rest[2 * len(levels) :]
    count = leaves * M
    part = count // CHUNKS
    half = devices // 2
    me = lax.axis_index("leaf")
    core, place = me % 2, me // 2
    has_before, has_after = me > 0, me < devices - 1
    twin = place * 2 + (1 - core)

    own_copy = pltpu.make_async_copy(charges_ref, own, local_sem.at[0])
    own_points = pltpu.make_async_copy(coords_ref, points.at[1], local_sem.at[1])
    near_copy = pltpu.make_async_copy(near_ref, named_leaves, local_sem.at[2])
    own_points.start()
    own_copy.start()
    near_copy.start()
    zeros_part[...] = jnp.zeros_like(zeros_part)

    def digit(stride, size):
        return (place // stride) % size

    def peer(stride, size, turn):
        mine = digit(stride, size)
        other = (mine + turn) % size
        return other, (place + (other - mine) * stride) * 2 + core

    barrier = pltpu.get_barrier_semaphore()
    met = 1
    pl.semaphore_signal(barrier, inc=1, device_id=(twin,), device_id_type=MESH)
    for stride, size in levels:
        for turn in range(1, size):
            met += 1
            pl.semaphore_signal(
                barrier, inc=1, device_id=(peer(stride, size, turn)[1],), device_id_type=MESH
            )

    @pl.when(has_before)
    def _():
        pl.semaphore_signal(barrier, inc=1, device_id=(me - 1,), device_id_type=MESH)

    @pl.when(has_after)
    def _():
        pl.semaphore_signal(barrier, inc=1, device_id=(me + 1,), device_id_type=MESH)

    pl.semaphore_wait(
        barrier, met + jnp.where(has_before, 1, 0) + jnp.where(has_after, 1, 0)
    )

    def remote(src, dst, send, recv, device):
        return pltpu.make_async_remote_copy(
            src_ref=src, dst_ref=dst, send_sem=send, recv_sem=recv,
            device_id=(device,), device_id_type=MESH,
        )

    def points_up():
        return remote(coords_ref, points.at[0], point_send.at[0], point_recv.at[0], me + 1)

    def points_down():
        return remote(coords_ref, points.at[2], point_send.at[1], point_recv.at[1], me - 1)

    def chunk_up(c):
        return remote(
            charges_ref.at[rows(c, part), :], before_ref.at[rows(c, part), :],
            up_send.at[c], near_recv.at[0], me + 1,
        )

    def chunk_down(c):
        return remote(
            charges_ref.at[rows(c, part), :], after_ref.at[rows(c, part), :],
            down_send.at[c], near_recv.at[1], me - 1,
        )

    def send_chunk(c):
        @pl.when(has_after)
        def _():
            chunk_up(c).start()

        @pl.when(has_before)
        def _():
            chunk_down(c).start()

    @pl.when(has_after)
    def _():
        points_up().start()

    @pl.when(has_before)
    def _():
        points_down().start()

    @pl.when(jnp.logical_not(has_before))
    def _():
        points[0] = jnp.zeros((3, count), F32)

    @pl.when(jnp.logical_not(has_after))
    def _():
        points[2] = jnp.zeros((3, count), F32)

    send_chunk(0)
    send_chunk(1)

    def fill(out_ref, sem):
        def each(c, carry):
            pltpu.make_async_copy(zeros_part, out_ref.at[rows(c, part), :], sem).start()
            return carry

        lax.fori_loop(0, CHUNKS, each, 0)

    def filled(out_ref, sem):
        pltpu.make_async_copy(own, out_ref, sem).wait()

    @pl.when(jnp.logical_not(has_before))
    def _():
        fill(before_ref, local_sem.at[3])

    @pl.when(jnp.logical_not(has_after))
    def _():
        fill(after_ref, local_sem.at[4])

    for p in range(K):
        basis[pl.ds(p, leaves, stride=K), :] = basis_ref[:, p * M : (p + 1) * M].astype(F32)
    basis_out[...] = basis[...].astype(BF16)
    spread(leaf_t, leaf_t_ref, leaves)
    spread(mid_t, mid_t_ref, leaves // 8)
    spread(base_t, base_t_ref, 1)

    own_copy.wait()

    def up_group(i, carry):
        for j in range(8):
            leaf = i * 8 + j
            coeffs[rows(leaf, K), :] = dot(
                basis_out[rows(leaf, K), :], own[rows(leaf, M), :]
            ).astype(BF16)
        return carry

    lax.fori_loop(0, leaves // 8, up_group, 0)
    mids = []
    for m in range(leaves // 8):
        area = slice(m * 8 * K, (m + 1) * 8 * K)
        mids.append(folded(dot_ta(leaf_t[area, :].astype(BF16), coeffs[area, :])).astype(BF16))
    base = folded(dot_ta(mid_t[...].astype(BF16), jnp.concatenate(mids, axis=0))).astype(BF16)
    spot = core * half + place
    gathered[spot] = jnp.concatenate(
        [base, folded(dot_ta(base_t[...].astype(BF16), base)).astype(BF16)], axis=0
    )

    def featured(which):
        def chunk(i, carry):
            first = pl.multiple_of(i * WIDTH, WIDTH)
            x = (points[which, :, pl.ds(first, WIDTH)] - 0.5) * scale
            h, m = halves(x)
            x = h + m
            norm = x[0:1] * x[0:1] + x[1:2] * x[1:2] + x[2:3] * x[2:3]
            ones = jnp.ones((3, WIDTH), F32)
            zeros = jnp.zeros((FEATURES - 18, WIDTH), F32)
            if which == 1:
                n = pieces(norm + DELTA_SQ * scale * scale)
                write_features(targets, first, WIDTH, [h, h, m, m, *n, ones, zeros])
            n = pieces(norm)
            h, m = -2.0 * h, -2.0 * m
            write_features(staged, 0, WIDTH, [h, m, h, m, ones, *n, zeros])
            for k in range(WIDTH // M):
                features[which * leaves + i * (WIDTH // M) + k] = staged[
                    :, k * M : (k + 1) * M
                ].astype(BF16)
            return carry

        lax.fori_loop(0, count // WIDTH, chunk, 0)

    def gather_copies(level):
        if level == len(levels):
            where = rows(core, half)
            return [remote(
                gathered.at[where], gathered.at[where],
                gather_send.at[level, 0], gather_recv.at[level, 0], twin,
            )]
        stride, size = levels[level]
        copies = []
        for turn in range(1, size):
            where = rows((core * half + place) // stride, stride)
            copies.append(remote(
                gathered.at[where], gathered.at[where],
                gather_send.at[level, turn - 1], gather_recv.at[level, turn - 1],
                peer(stride, size, turn)[1],
            ))
        return copies

    def reduce_copies(level):
        if level == len(levels):
            return [remote(
                partial.at[rows(1 - core, half * 2 * K), :], core_got,
                reduce_send.at[level, 0], reduce_recv.at[level, 0], twin,
            )]
        stride, size = levels[level]
        copies = []
        for turn in range(1, size):
            other, device = peer(stride, size, turn)
            copies.append(remote(
                currents[level].at[rows(other, stride * 2 * K), :], receives[level].at[turn - 1],
                reduce_send.at[level, turn - 1], reduce_recv.at[level, turn - 1], device,
            ))
        return copies

    def start(copies):
        for copy in copies:
            copy.start()

    def arrived(copies):
        for copy in copies:
            copy.wait_recv()

    def sent(copies):
        for copy in copies:
            copy.wait_send()

    def spot_of(device):
        return (device % 2) * half + device // 2

    def couple():
        for t in range(devices // 8):
            total = jnp.zeros((K, RHS), F32)
            for j in range(8):
                total = total + gathered[spot_of(t * 8 + j), K:, :].astype(F32)
            top_coeffs[t] = total.astype(BF16)

        for d in range(devices):
            wide[d] = tiled(gathered[d, :K, :])

        def group(i, carry):
            for j in range(step):
                b = i * step + j
                source = source_ref[b]
                where = (source & 1) * half + (source >> 1)
                products[rows(b, K), :] = dot(
                    products[rows(b, K), :].astype(BF16), wide[where]
                )
            return carry

        lax.fori_loop(0, blocks // step, group, 0)
        named_spot = target_ref[...]
        named_spot = (named_spot & 1) * half + (named_spot >> 1)
        ids = lax.broadcasted_iota(jnp.int32, (devices, blocks), 0)
        chosen = jnp.where(ids == named_spot, 1.0, 0.0).astype(BF16)

        def scatter(i, carry):
            for j in range(8):
                k = i * 8 + j
                terms = products[pl.ds(k, blocks, stride=K), :].astype(BF16)
                partial[pl.ds(k, devices, stride=2 * K), :] = dot(chosen, terms)
            return carry

        lax.fori_loop(0, K // 8, scatter, 0)
        terms = [
            dot(top_t[b * K : (b + 1) * K, :].astype(BF16), tiled(top_coeffs[top_source_ref[b]]))
            for b in range(top_blocks)
        ]
        for t in range(devices // 8):
            total = jnp.zeros((K, RHS), F32)
            for b in range(top_blocks):
                total = total + jnp.where(top_target_ref[b] == t, 1.0, 0.0) * terms[b]
            for j in range(8):
                first = spot_of(t * 8 + j) * 2 * K + K
                partial[first : first + K, :] = total

    def reduced_core():
        mine = partial[rows(core, half * 2 * K), :]
        currents[-1][...] = (mine + core_got[...]).astype(BF16)

    def reduced(level):
        stride, size = levels[level]
        total = currents[level][rows(digit(stride, size), stride * 2 * K), :].astype(F32)
        for turn in range(1, size):
            total = total + receives[level][turn - 1].astype(F32)
        return total

    own_points.wait()
    near_copy.wait()
    featured(1)
    start(gather_copies(0))
    spread(products, blocks_ref, blocks)
    spread(top_t, top_blocks_ref, top_blocks)
    send_chunk(2)

    @pl.when(has_before)
    def _():
        points_up().wait_recv()

    @pl.when(has_after)
    def _():
        points_down().wait_recv()

    featured(0)
    featured(2)
    send_chunk(3)

    stages = []
    for level in range(len(levels)):
        def gather(level=level):
            arrived(gather_copies(level))
            start(gather_copies(level + 1))
        stages.append((3 * level, gather))
    at = 3 * len(levels)

    def coupled():
        arrived(gather_copies(len(levels)))
        couple()

    stages.append((at, coupled))
    stages.append((at + 1, lambda: start(reduce_copies(len(levels)))))

    def core_reduced():
        arrived(reduce_copies(len(levels)))
        reduced_core()

    stages.append((at + 4, core_reduced))
    at += 5
    for level in range(len(levels) - 1, -1, -1):
        stages.append((at, lambda level=level: start(reduce_copies(level))))
        if level:
            def reduce(level=level):
                arrived(reduce_copies(level))
                currents[level - 1][...] = reduced(level).astype(BF16)
            stages.append((at + 3, reduce))
        at += 4

    def made_copy(i, slot):
        return pltpu.make_async_copy(
            made.at[slot], kernels_ref.at[pl.ds(i * EACH, EACH)], made_sem.at[slot]
        )

    steps = leaves // EACH

    def make(i, carry):
        for when, stage in stages:
            pl.when(i == when)(stage)

        @pl.when((i % 2 == 0) & (i < 2 * (CHUNKS - 4)))
        def _():
            send_chunk(4 + i // 2)

        slot = i % 2

        @pl.when(i >= 2)
        def _():
            made_copy(i - 2, slot).wait()

        for k in range(EACH):
            leaf = i * EACH + k
            mine = targets[:, rows(leaf, M)].T.astype(BF16)
            for group in groups_of(named):
                theirs = jnp.concatenate(
                    [features[named_leaves[j, leaf]] for j in group], axis=1
                )
                squares = dot(mine, theirs)
                made[slot, k, :, group[0] * M : (group[-1] + 1) * M] = lax.rsqrt(
                    squares.astype(BF16)
                )
        made_copy(i, slot).start()
        return carry

    lax.fori_loop(0, steps, make, 0)
    arrived(reduce_copies(0))
    total = reduced(0)
    base = (
        total[:K] + dot(base_t[...].astype(BF16), tiled(total[K:].astype(BF16)))
    ).astype(BF16)
    mid = dot(mid_t[...].astype(BF16), tiled(base)).astype(BF16)
    for m in range(leaves // 8):
        area = slice(m * 8 * K, (m + 1) * 8 * K)
        fields_ref[area, :] = dot(
            leaf_t[area, :].astype(BF16), tiled(mid[m * K : (m + 1) * K, :])
        ).astype(BF16)

    made_copy(steps - 2, steps % 2).wait()
    made_copy(steps - 1, (steps - 1) % 2).wait()

    for level in range(len(levels) + 1):
        sent(gather_copies(level))
        sent(reduce_copies(level))

    def drain_up(c, carry):
        chunk_up(c).wait_send()
        return carry

    def drain_down(c, carry):
        chunk_down(c).wait_send()
        return carry

    @pl.when(has_after)
    def _():
        points_up().wait_send()
        lax.fori_loop(0, CHUNKS, drain_up, 0)
        remote(charges_ref, after_ref, up_send.at[0], near_recv.at[1], me + 1).wait_recv()

    @pl.when(has_before)
    def _():
        points_down().wait_send()
        lax.fori_loop(0, CHUNKS, drain_down, 0)
        remote(charges_ref, before_ref, up_send.at[0], near_recv.at[0], me - 1).wait_recv()

    @pl.when(jnp.logical_not(has_before))
    def _():
        filled(before_ref, local_sem.at[3])

    @pl.when(jnp.logical_not(has_after))
    def _():
        filled(after_ref, local_sem.at[4])


def use_kernel(
    leaves, named,
    near_ref, kernel_ref, before_ref, own_ref, after_ref, fields_ref, basis_ref, out_ref,
    pool, sems,
):
    points = leaves * M

    @pl.when(pl.program_id(0) == 0)
    def _():
        copies = [
            pltpu.make_async_copy(ref, pool.at[pl.ds(i * points, points), :], sems.at[i])
            for i, ref in enumerate((before_ref, own_ref, after_ref))
        ]
        for copy in copies:
            copy.start()
        for copy in copies:
            copy.wait()

    for k in range(kernel_ref.shape[0]):
        leaf = pl.program_id(0) * kernel_ref.shape[0] + k
        total = dot_ta(basis_ref[rows(leaf, K), :], fields_ref[rows(leaf, K), :])
        for group in groups_of(named):
            theirs = jnp.concatenate([pool[rows(near_ref[j, leaf], M), :] for j in group], axis=0)
            total = total + dot(kernel_ref[k, :, group[0] * M : (group[-1] + 1) * M], theirs)
        out_ref[k * M : (k + 1) * M, :] = total.astype(BF16)


def per_device(
    coords,
    charges,
    near_leaves,
    leaf_basis,
    leaf_transfer,
    mid_transfer,
    base_transfer,
    base_coupling,
    base_target,
    base_source,
    top_coupling,
    top_target,
    top_source,
):
    leaves, named = near_leaves.shape
    devices = lax.axis_size("leaf")
    blocks, top_blocks = base_coupling.shape[0], top_coupling.shape[0]
    scale = math.sqrt(named * M)
    count = leaves * M
    half = devices // 2
    levels = levels_of(devices)
    widest = max(size for _, size in levels)
    step = max(s for s in range(1, 33) if blocks % s == 0)
    kernels, before, after, fields, basis = pl.pallas_call(
        functools.partial(
            exchange_kernel, devices, leaves, named, blocks, top_blocks, step, scale
        ),
        out_shape=[
            jax.ShapeDtypeStruct((leaves, M, named * M), BF16),
            jax.ShapeDtypeStruct((count, RHS), BF16),
            jax.ShapeDtypeStruct((count, RHS), BF16),
            jax.ShapeDtypeStruct((leaves * K, RHS), BF16),
            jax.ShapeDtypeStruct((leaves * K, M), BF16),
        ],
        in_specs=[SMEM] * 3 + [ANY] * 3 + [VMEM] * 7,
        out_specs=[ANY] * 3 + [VMEM] * 2,
        scratch_shapes=[
            pltpu.SMEM((named, leaves), jnp.int32),
            pltpu.VMEM((3, 3, count), F32),
            pltpu.VMEM((count, RHS), BF16),
            pltpu.VMEM((3 * leaves, FEATURES, M), BF16),
            pltpu.VMEM((FEATURES, count), F32),
            pltpu.VMEM((FEATURES, WIDTH), F32),
            pltpu.VMEM((2, EACH, M, named * M), BF16),
            pltpu.VMEM((leaves * K, RHS), BF16),
            pltpu.VMEM((devices, 2 * K, RHS), BF16),
            pltpu.VMEM((count // CHUNKS, RHS), BF16),
            pltpu.VMEM((leaves * K, M), F32),
            pltpu.VMEM((leaves * K, LANES), F32),
            pltpu.VMEM((leaves // 8 * K, LANES), F32),
            pltpu.VMEM((K, LANES), F32),
            pltpu.VMEM((top_blocks * K, LANES), F32),
            pltpu.VMEM((devices, LANES, RHS), BF16),
            pltpu.VMEM((blocks * K, RHS), F32),
            pltpu.VMEM((devices * 2 * K, RHS), F32),
            pltpu.VMEM((half * 2 * K, RHS), F32),
            pltpu.VMEM((devices // 8, K, RHS), BF16),
        ]
        + [pltpu.VMEM((stride * size * 2 * K, RHS), BF16) for stride, size in levels]
        + [pltpu.VMEM((size - 1, stride * 2 * K, RHS), BF16) for stride, size in levels]
        + [
            pltpu.SemaphoreType.DMA((5,)),
            pltpu.SemaphoreType.DMA((2,)),
            pltpu.SemaphoreType.DMA((2,)),
            pltpu.SemaphoreType.DMA((2,)),
            pltpu.SemaphoreType.DMA((CHUNKS,)),
            pltpu.SemaphoreType.DMA((CHUNKS,)),
            pltpu.SemaphoreType.DMA((2,)),
        ]
        + [pltpu.SemaphoreType.DMA((len(levels) + 1, widest - 1))] * 4,
        compiler_params=pltpu.CompilerParams(
            vmem_limit_bytes=60 * 1024 * 1024, collective_id=0, has_side_effects=True
        ),
        cost_estimate=pl.CostEstimate(
            flops=16_000_000_000, bytes_accessed=70_000_000, transcendentals=28_000_000
        ),
        name="exchange",
    )(
        base_source, top_target, top_source, near_leaves.T, coords, charges,
        base_target.T, leaf_basis, leaf_transfer, mid_transfer, base_transfer,
        base_coupling, top_coupling,
    )
    each = 4
    return pl.pallas_call(
        functools.partial(use_kernel, leaves, named),
        grid=(leaves // each,),
        out_shape=jax.ShapeDtypeStruct((count, RHS), BF16),
        in_specs=[SMEM, pl.BlockSpec((each, M, named * M), lambda i: (i, 0, 0)), ANY, ANY, ANY]
        + [VMEM] * 2,
        out_specs=pl.BlockSpec((each * M, RHS), lambda i: (i, 0)),
        scratch_shapes=[
            pltpu.VMEM((3 * count, RHS), BF16),
            pltpu.SemaphoreType.DMA((3,)),
        ],
        compiler_params=pltpu.CompilerParams(vmem_limit_bytes=60 * 1024 * 1024),
        cost_estimate=pl.CostEstimate(
            flops=8_000_000_000, bytes_accessed=66_000_000, transcendentals=0
        ),
        name="use",
    )(near_leaves.T, kernels, before, charges, after, fields, basis)


def solution(mesh):
    split, flat = P("leaf", None), P("leaf")
    in_specs = (P(None, "leaf"),) + (split,) * 8 + (flat, split, flat, flat)
    return jax.shard_map(
        per_device, mesh=mesh, in_specs=in_specs, out_specs=split, check_vma=False
    )
```

```python
import functools
import math

import jax
import jax.numpy as jnp
from jax import lax
from jax.experimental import pallas as pl
from jax.experimental.pallas import tpu as pltpu
from jax.sharding import PartitionSpec as P

K = 32
RHS = 128
M = 128
FEATURES = 32
DELTA_SQ = 0.0025
CHUNKS = 16
EACH = 4
KEEP = 36
WIDTH = 2048
LANES = 128
FOLD = LANES // K

F32 = jnp.float32
BF16 = jnp.bfloat16
MESH = pl.DeviceIdType.MESH
VMEM = pl.BlockSpec(memory_space=pltpu.VMEM)
SMEM = pl.BlockSpec(memory_space=pltpu.SMEM)
ANY = pl.BlockSpec(memory_space=pl.ANY)


def dot(a, b):
    return jnp.dot(a, b, preferred_element_type=F32)


def dot_ta(a, b):
    return lax.dot_general(a, b, (((0,), (0,)), ((), ())), preferred_element_type=F32)


def rows(index, size):
    return pl.ds(pl.multiple_of(index * size, size), size)


def halves(x):
    high = x.astype(BF16).astype(F32)
    return high, (x - high).astype(BF16).astype(F32)


def spread(dst, src, count):
    lane = lax.broadcasted_iota(jnp.int32, (1, LANES), 1) // K
    masks = [jnp.where(lane == f, 1.0, 0.0) for f in range(FOLD)]
    for tile in range(K // FOLD):
        slab = src[:, tile * LANES : (tile + 1) * LANES].astype(F32)
        for f in range(FOLD):
            dst[pl.ds(tile * FOLD + f, count, stride=K), :] = slab * masks[f]


def folded(x):
    return sum(x[f * K : (f + 1) * K, :] for f in range(1, FOLD)) + x[:K, :]


def tiled(x):
    return jnp.concatenate([x] * FOLD, axis=0)


def pieces(x):
    high = x.astype(BF16).astype(F32)
    rest = x - high
    middle = rest.astype(BF16).astype(F32)
    return high, middle, (rest - middle).astype(BF16).astype(F32)


def write_features(rows_ref, first, width, parts):
    at = 0
    for part in parts:
        rows_ref[at : at + part.shape[0], pl.ds(first, width)] = part
        at += part.shape[0]


def groups_of(named):
    return [range(j, min(j + 2, named)) for j in range(0, named, 2)]


def levels_of(devices):
    half = devices // 2
    low = 2 ** (int(math.log2(half // 4)) // 2)
    levels, stride = [], 1
    for size in (low, half // 4 // low, 4):
        levels.append((stride, size))
        stride *= size
    return levels


def exchange_kernel(
    devices, leaves, named, blocks, top_blocks, step, scale,
    source_ref, top_target_ref, top_source_ref,
    near_ref, coords_ref, charges_ref,
    target_ref, basis_ref, leaf_t_ref, mid_t_ref, base_t_ref, blocks_ref, top_blocks_ref,
    out_ref, spill_ref,
    named_leaves, points, pool, slots, outs, fields, basis_out, features, targets, staged, coeffs, gathered,
    basis, leaf_t, mid_t, base_t, top_t, wide, products, partial, core_got,
    top_coeffs, *rest,
):
    levels = levels_of(devices)
    currents, receives = rest[: len(levels)], rest[len(levels) : 2 * len(levels)]
    (local_sem, spill_sem, fill_sem, out_sem, point_send, point_recv, up_send, down_send, near_recv,
     gather_send, gather_recv, reduce_send, reduce_recv) = rest[2 * len(levels) :]
    count = leaves * M
    part = leaves // CHUNKS
    half = devices // 2
    me = lax.axis_index("leaf")
    core, place = me % 2, me // 2
    has_before, has_after = me > 0, me < devices - 1
    twin = place * 2 + (1 - core)

    own_copy = pltpu.make_async_copy(charges_ref, pool.at[pl.ds(leaves, leaves)], local_sem.at[0])
    own_points = pltpu.make_async_copy(coords_ref, points.at[1], local_sem.at[1])
    near_copy = pltpu.make_async_copy(near_ref, named_leaves, local_sem.at[2])
    own_points.start()
    own_copy.start()
    near_copy.start()

    def digit(stride, size):
        return (place // stride) % size

    def peer(stride, size, turn):
        mine = digit(stride, size)
        other = (mine + turn) % size
        return other, (place + (other - mine) * stride) * 2 + core

    barrier = pltpu.get_barrier_semaphore()
    met = 1
    pl.semaphore_signal(barrier, inc=1, device_id=(twin,), device_id_type=MESH)
    for stride, size in levels:
        for turn in range(1, size):
            met += 1
            pl.semaphore_signal(
                barrier, inc=1, device_id=(peer(stride, size, turn)[1],), device_id_type=MESH
            )

    @pl.when(has_before)
    def _():
        pl.semaphore_signal(barrier, inc=1, device_id=(me - 1,), device_id_type=MESH)

    @pl.when(has_after)
    def _():
        pl.semaphore_signal(barrier, inc=1, device_id=(me + 1,), device_id_type=MESH)

    pl.semaphore_wait(
        barrier, met + jnp.where(has_before, 1, 0) + jnp.where(has_after, 1, 0)
    )

    def remote(src, dst, send, recv, device):
        return pltpu.make_async_remote_copy(
            src_ref=src, dst_ref=dst, send_sem=send, recv_sem=recv,
            device_id=(device,), device_id_type=MESH,
        )

    def points_up():
        return remote(coords_ref, points.at[0], point_send.at[0], point_recv.at[0], me + 1)

    def points_down():
        return remote(coords_ref, points.at[2], point_send.at[1], point_recv.at[1], me - 1)

    def chunk_up(c):
        return remote(
            charges_ref.at[rows(c, part)], pool.at[rows(c, part)],
            up_send.at[c], near_recv.at[0], me + 1,
        )

    def chunk_down(c):
        return remote(
            charges_ref.at[rows(c, part)], pool.at[rows(2 * CHUNKS + c, part)],
            down_send.at[c], near_recv.at[1], me - 1,
        )

    def send_chunk(c):
        @pl.when(has_after)
        def _():
            chunk_up(c).start()

        @pl.when(has_before)
        def _():
            chunk_down(c).start()

    @pl.when(has_after)
    def _():
        points_up().start()

    @pl.when(has_before)
    def _():
        points_down().start()

    @pl.when(jnp.logical_not(has_before))
    def _():
        points[0] = jnp.zeros((3, count), F32)
        pool[:leaves] = jnp.zeros((leaves, M, RHS), BF16)

    @pl.when(jnp.logical_not(has_after))
    def _():
        points[2] = jnp.zeros((3, count), F32)
        pool[2 * leaves :] = jnp.zeros((leaves, M, RHS), BF16)

    send_chunk(0)
    send_chunk(1)

    for p in range(K):
        basis[pl.ds(p, leaves, stride=K), :] = basis_ref[:, p * M : (p + 1) * M].astype(F32)
    basis_out[...] = basis[...].astype(BF16)
    spread(leaf_t, leaf_t_ref, leaves)
    spread(mid_t, mid_t_ref, leaves // 8)
    spread(base_t, base_t_ref, 1)

    own_copy.wait()

    def up_group(i, carry):
        for j in range(8):
            leaf = i * 8 + j
            coeffs[rows(leaf, K), :] = dot(
                basis_out[rows(leaf, K), :], pool[leaves + leaf]
            ).astype(BF16)
        return carry

    lax.fori_loop(0, leaves // 8, up_group, 0)
    mids = []
    for m in range(leaves // 8):
        area = slice(m * 8 * K, (m + 1) * 8 * K)
        mids.append(folded(dot_ta(leaf_t[area, :].astype(BF16), coeffs[area, :])).astype(BF16))
    base = folded(dot_ta(mid_t[...].astype(BF16), jnp.concatenate(mids, axis=0))).astype(BF16)
    spot = core * half + place
    gathered[spot] = jnp.concatenate(
        [base, folded(dot_ta(base_t[...].astype(BF16), base)).astype(BF16)], axis=0
    )

    def featured(which):
        def chunk(i, carry):
            first = pl.multiple_of(i * WIDTH, WIDTH)
            x = (points[which, :, pl.ds(first, WIDTH)] - 0.5) * scale
            h, m = halves(x)
            x = h + m
            norm = x[0:1] * x[0:1] + x[1:2] * x[1:2] + x[2:3] * x[2:3]
            ones = jnp.ones((3, WIDTH), F32)
            zeros = jnp.zeros((FEATURES - 18, WIDTH), F32)
            if which == 1:
                n = pieces(norm + DELTA_SQ * scale * scale)
                write_features(targets, first, WIDTH, [h, h, m, m, *n, ones, zeros])
            n = pieces(norm)
            h, m = -2.0 * h, -2.0 * m
            write_features(staged, 0, WIDTH, [h, m, h, m, ones, *n, zeros])
            for k in range(WIDTH // M):
                features[which * leaves + i * (WIDTH // M) + k] = staged[
                    :, k * M : (k + 1) * M
                ].astype(BF16)
            return carry

        lax.fori_loop(0, count // WIDTH, chunk, 0)

    def gather_copies(level):
        if level == len(levels):
            where = rows(core, half)
            return [remote(
                gathered.at[where], gathered.at[where],
                gather_send.at[level, 0], gather_recv.at[level, 0], twin,
            )]
        stride, size = levels[level]
        copies = []
        for turn in range(1, size):
            where = rows((core * half + place) // stride, stride)
            copies.append(remote(
                gathered.at[where], gathered.at[where],
                gather_send.at[level, turn - 1], gather_recv.at[level, turn - 1],
                peer(stride, size, turn)[1],
            ))
        return copies

    def reduce_copies(level):
        if level == len(levels):
            return [remote(
                partial.at[rows(1 - core, half * 2 * K), :], core_got,
                reduce_send.at[level, 0], reduce_recv.at[level, 0], twin,
            )]
        stride, size = levels[level]
        copies = []
        for turn in range(1, size):
            other, device = peer(stride, size, turn)
            copies.append(remote(
                currents[level].at[rows(other, stride * 2 * K), :], receives[level].at[turn - 1],
                reduce_send.at[level, turn - 1], reduce_recv.at[level, turn - 1], device,
            ))
        return copies

    def start(copies):
        for copy in copies:
            copy.start()

    def arrived(copies):
        for copy in copies:
            copy.wait_recv()

    def sent(copies):
        for copy in copies:
            copy.wait_send()

    def spot_of(device):
        return (device % 2) * half + device // 2

    def couple():
        for t in range(devices // 8):
            total = jnp.zeros((K, RHS), F32)
            for j in range(8):
                total = total + gathered[spot_of(t * 8 + j), K:, :].astype(F32)
            top_coeffs[t] = total.astype(BF16)

        for d in range(devices):
            wide[d] = tiled(gathered[d, :K, :])

        def group(i, carry):
            for j in range(step):
                b = i * step + j
                source = source_ref[b]
                where = (source & 1) * half + (source >> 1)
                products[rows(b, K), :] = dot(
                    products[rows(b, K), :].astype(BF16), wide[where]
                )
            return carry

        lax.fori_loop(0, blocks // step, group, 0)
        named_spot = target_ref[...]
        named_spot = (named_spot & 1) * half + (named_spot >> 1)
        ids = lax.broadcasted_iota(jnp.int32, (devices, blocks), 0)
        chosen = jnp.where(ids == named_spot, 1.0, 0.0).astype(BF16)

        def scatter(i, carry):
            for j in range(8):
                k = i * 8 + j
                terms = products[pl.ds(k, blocks, stride=K), :].astype(BF16)
                partial[pl.ds(k, devices, stride=2 * K), :] = dot(chosen, terms)
            return carry

        lax.fori_loop(0, K // 8, scatter, 0)
        terms = [
            dot(top_t[b * K : (b + 1) * K, :].astype(BF16), tiled(top_coeffs[top_source_ref[b]]))
            for b in range(top_blocks)
        ]
        for t in range(devices // 8):
            total = jnp.zeros((K, RHS), F32)
            for b in range(top_blocks):
                total = total + jnp.where(top_target_ref[b] == t, 1.0, 0.0) * terms[b]
            for j in range(8):
                first = spot_of(t * 8 + j) * 2 * K + K
                partial[first : first + K, :] = total

    def reduced_core():
        mine = partial[rows(core, half * 2 * K), :]
        currents[-1][...] = (mine + core_got[...]).astype(BF16)

    def reduced(level):
        stride, size = levels[level]
        total = currents[level][rows(digit(stride, size), stride * 2 * K), :].astype(F32)
        for turn in range(1, size):
            total = total + receives[level][turn - 1].astype(F32)
        return total

    own_points.wait()
    near_copy.wait()
    featured(1)
    start(gather_copies(0))
    spread(products, blocks_ref, blocks)
    spread(top_t, top_blocks_ref, top_blocks)
    send_chunk(2)

    @pl.when(has_before)
    def _():
        points_up().wait_recv()

    @pl.when(has_after)
    def _():
        points_down().wait_recv()

    featured(0)
    featured(2)
    send_chunk(3)

    stages = []
    for level in range(len(levels)):
        def gather(level=level):
            arrived(gather_copies(level))
            start(gather_copies(level + 1))
        stages.append((level, gather))

    def coupled():
        arrived(gather_copies(len(levels)))
        couple()

    def core_reduced():
        arrived(reduce_copies(len(levels)))
        reduced_core()

    stages.append((3, coupled))
    stages.append((4, lambda: start(reduce_copies(len(levels)))))
    stages.append((5, core_reduced))
    at = 6
    for level in range(len(levels) - 1, -1, -1):
        stages.append((at, lambda level=level: start(reduce_copies(level))))
        if level:
            def reduce(level=level):
                arrived(reduce_copies(level))
                currents[level - 1][...] = reduced(level).astype(BF16)
            stages.append((at + 1, reduce))
        at += 2

    steps, kept = leaves // EACH, KEEP // EACH
    spilled = steps - kept

    def spill_copy(i):
        return pltpu.make_async_copy(
            slots.at[rows(i, EACH)], spill_ref.at[rows(i, EACH)], spill_sem.at[i]
        )

    def fill_copy(i):
        return pltpu.make_async_copy(
            spill_ref.at[rows(i, EACH)], slots.at[rows(i, EACH)], fill_sem.at[i]
        )

    def out_copy(step, slot):
        return pltpu.make_async_copy(
            outs.at[slot], out_ref.at[rows(step, EACH * M), :], out_sem.at[slot]
        )

    def make(i, carry):
        for when, stage in stages:
            pl.when(i == when)(stage)

        @pl.when((i < 8) | (i % 2 == 1))
        def _():
            send_chunk(4 + jnp.where(i < 8, i, 8 + (i - 9) // 2))

        @pl.when(i >= kept)
        def _():
            spill_copy(i - kept).wait()

        for k in range(EACH):
            leaf = i * EACH + k
            mine = targets[:, rows(leaf, M)].T.astype(BF16)
            theirs = jnp.concatenate(
                [features[named_leaves[j, leaf]] for j in range(named)], axis=1
            )
            slots[(i % kept) * EACH + k] = lax.rsqrt(dot(mine, theirs).astype(BF16))

        @pl.when(i < spilled)
        def _():
            spill_copy(i).start()

        return carry

    lax.fori_loop(0, steps, make, 0)
    arrived(reduce_copies(0))
    total = reduced(0)
    base = (
        total[:K] + dot(base_t[...].astype(BF16), tiled(total[K:].astype(BF16)))
    ).astype(BF16)
    mid = dot(mid_t[...].astype(BF16), tiled(base)).astype(BF16)
    for m in range(leaves // 8):
        area = slice(m * 8 * K, (m + 1) * 8 * K)
        fields[area, :] = dot(
            leaf_t[area, :].astype(BF16), tiled(mid[m * K : (m + 1) * K, :])
        ).astype(BF16)

    @pl.when(has_after)
    def _():
        remote(
            charges_ref, pool.at[pl.ds(2 * leaves, leaves)], up_send.at[0], near_recv.at[1], me + 1
        ).wait_recv()

    @pl.when(has_before)
    def _():
        remote(
            charges_ref, pool.at[pl.ds(0, leaves)], up_send.at[0], near_recv.at[0], me - 1
        ).wait_recv()

    def use(i, carry):
        block = jnp.where(i < spilled, i + kept, jnp.where(i < kept, i, i - kept))
        slot = i % 2

        @pl.when(i >= kept)
        def _():
            fill_copy(i - kept).wait()

        @pl.when(i >= 2)
        def _():
            out_copy(i, slot).wait()

        for k in range(EACH):
            leaf = block * EACH + k
            near = jnp.concatenate(
                [pool[named_leaves[j, leaf]] for j in range(named)], axis=0
            )
            total = dot(slots[(i % kept) * EACH + k], near)
            total = total + dot_ta(basis_out[rows(leaf, K), :], fields[rows(leaf, K), :])
            outs[slot, k * M : (k + 1) * M, :] = total.astype(BF16)
        out_copy(block, slot).start()

        @pl.when(i < spilled)
        def _():
            fill_copy(i).start()

        return carry

    lax.fori_loop(0, steps, use, 0)
    out_copy(0, 0).wait()
    out_copy(1, 1).wait()

    for level in range(len(levels) + 1):
        sent(gather_copies(level))
        sent(reduce_copies(level))

    def drain_up(c, carry):
        chunk_up(c).wait_send()
        return carry

    def drain_down(c, carry):
        chunk_down(c).wait_send()
        return carry

    @pl.when(has_after)
    def _():
        points_up().wait_send()
        lax.fori_loop(0, CHUNKS, drain_up, 0)

    @pl.when(has_before)
    def _():
        points_down().wait_send()
        lax.fori_loop(0, CHUNKS, drain_down, 0)


def per_device(
    coords,
    charges,
    near_leaves,
    leaf_basis,
    leaf_transfer,
    mid_transfer,
    base_transfer,
    base_coupling,
    base_target,
    base_source,
    top_coupling,
    top_target,
    top_source,
):
    leaves, named = near_leaves.shape
    devices = lax.axis_size("leaf")
    blocks, top_blocks = base_coupling.shape[0], top_coupling.shape[0]
    scale = math.sqrt(named * M)
    count = leaves * M
    half = devices // 2
    levels = levels_of(devices)
    widest = max(size for _, size in levels)
    step = max(s for s in range(1, 33) if blocks % s == 0)
    out, _ = pl.pallas_call(
        functools.partial(
            exchange_kernel, devices, leaves, named, blocks, top_blocks, step, scale
        ),
        out_shape=[
            jax.ShapeDtypeStruct((count, RHS), BF16),
            jax.ShapeDtypeStruct((leaves - KEEP, M, named * M), BF16),
        ],
        in_specs=[SMEM] * 3 + [ANY] * 3 + [VMEM] * 7,
        out_specs=[ANY] * 2,
        scratch_shapes=[
            pltpu.SMEM((named, leaves), jnp.int32),
            pltpu.VMEM((3, 3, count), F32),
            pltpu.VMEM((3 * leaves, M, RHS), BF16),
            pltpu.VMEM((KEEP, M, named * M), BF16),
            pltpu.VMEM((2, EACH * M, RHS), BF16),
            pltpu.VMEM((leaves * K, RHS), BF16),
            pltpu.VMEM((leaves * K, M), BF16),
            pltpu.VMEM((3 * leaves, FEATURES, M), BF16),
            pltpu.VMEM((FEATURES, count), F32),
            pltpu.VMEM((FEATURES, WIDTH), F32),
            pltpu.VMEM((leaves * K, RHS), BF16),
            pltpu.VMEM((devices, 2 * K, RHS), BF16),
            pltpu.VMEM((leaves * K, M), F32),
            pltpu.VMEM((leaves * K, LANES), F32),
            pltpu.VMEM((leaves // 8 * K, LANES), F32),
            pltpu.VMEM((K, LANES), F32),
            pltpu.VMEM((top_blocks * K, LANES), F32),
            pltpu.VMEM((devices, LANES, RHS), BF16),
            pltpu.VMEM((blocks * K, RHS), F32),
            pltpu.VMEM((devices * 2 * K, RHS), F32),
            pltpu.VMEM((half * 2 * K, RHS), F32),
            pltpu.VMEM((devices // 8, K, RHS), BF16),
        ]
        + [pltpu.VMEM((stride * size * 2 * K, RHS), BF16) for stride, size in levels]
        + [pltpu.VMEM((size - 1, stride * 2 * K, RHS), BF16) for stride, size in levels]
        + [
            pltpu.SemaphoreType.DMA((3,)),
            pltpu.SemaphoreType.DMA(((leaves - KEEP) // EACH,)),
            pltpu.SemaphoreType.DMA(((leaves - KEEP) // EACH,)),
            pltpu.SemaphoreType.DMA((2,)),
            pltpu.SemaphoreType.DMA((2,)),
            pltpu.SemaphoreType.DMA((2,)),
            pltpu.SemaphoreType.DMA((CHUNKS,)),
            pltpu.SemaphoreType.DMA((CHUNKS,)),
            pltpu.SemaphoreType.DMA((2,)),
        ]
        + [pltpu.SemaphoreType.DMA((len(levels) + 1, widest - 1))] * 4,
        compiler_params=pltpu.CompilerParams(
            vmem_limit_bytes=63 * 1024 * 1024, collective_id=0, has_side_effects=True
        ),
        cost_estimate=pl.CostEstimate(
            flops=16_000_000_000, bytes_accessed=70_000_000, transcendentals=28_000_000
        ),
        name="exchange",
    )(
        base_source, top_target, top_source, near_leaves.T, coords,
        charges.reshape(leaves, M, RHS),
        base_target.T, leaf_basis, leaf_transfer, mid_transfer, base_transfer,
        base_coupling, top_coupling,
    )
    return out


def solution(mesh):
    split, flat = P("leaf", None), P("leaf")
    in_specs = (P(None, "leaf"),) + (split,) * 8 + (flat, split, flat, flat)
    return jax.shard_map(
        per_device, mesh=mesh, in_specs=in_specs, out_specs=split, check_vma=False
    )
```

```python
import functools
import math

import jax
import jax.numpy as jnp
from jax import lax
from jax.experimental import pallas as pl
from jax.experimental.pallas import tpu as pltpu
from jax.sharding import PartitionSpec as P

K = 32
RHS = 128
M = 128
FEATURES = 32
DELTA_SQ = 0.0025
CHUNKS = 16
EACH = 4
KEEP = 36
WIDTH = 2048
LANES = 128
FOLD = LANES // K

F32 = jnp.float32
BF16 = jnp.bfloat16
MESH = pl.DeviceIdType.MESH
VMEM = pl.BlockSpec(memory_space=pltpu.VMEM)
SMEM = pl.BlockSpec(memory_space=pltpu.SMEM)
ANY = pl.BlockSpec(memory_space=pl.ANY)


def dot(a, b):
    return jnp.dot(a, b, preferred_element_type=F32)


def dot_ta(a, b):
    return lax.dot_general(a, b, (((0,), (0,)), ((), ())), preferred_element_type=F32)


def rows(index, size):
    return pl.ds(pl.multiple_of(index * size, size), size)


def halves(x):
    high = x.astype(BF16).astype(F32)
    return high, (x - high).astype(BF16).astype(F32)


def spread(dst, src, count):
    lane = lax.broadcasted_iota(jnp.int32, (1, LANES), 1) // K
    masks = [jnp.where(lane == f, 1.0, 0.0) for f in range(FOLD)]
    for tile in range(K // FOLD):
        slab = src[:, tile * LANES : (tile + 1) * LANES].astype(F32)
        for f in range(FOLD):
            dst[pl.ds(tile * FOLD + f, count, stride=K), :] = slab * masks[f]


def folded(x):
    return sum(x[f * K : (f + 1) * K, :] for f in range(1, FOLD)) + x[:K, :]


def tiled(x):
    return jnp.concatenate([x] * FOLD, axis=0)


def pieces(x):
    high = x.astype(BF16).astype(F32)
    rest = x - high
    middle = rest.astype(BF16).astype(F32)
    return high, middle, (rest - middle).astype(BF16).astype(F32)


def write_features(rows_ref, first, width, parts):
    at = 0
    for part in parts:
        rows_ref[at : at + part.shape[0], pl.ds(first, width)] = part
        at += part.shape[0]


def groups_of(named):
    return [range(j, min(j + 2, named)) for j in range(0, named, 2)]


def levels_of(devices):
    plane = devices // 8
    if plane <= 4:
        return [(1, plane), (plane, 4)]
    low = 2 ** (int(math.log2(plane)) // 2)
    return [(1, low), (low, plane // low), (plane, 4)]


def exchange_kernel(
    devices, leaves, named, blocks, top_blocks, step, scale,
    source_ref, top_target_ref, top_source_ref,
    near_ref, coords_ref, charges_ref,
    target_ref, basis_ref, leaf_t_ref, mid_t_ref, base_t_ref, blocks_ref, top_blocks_ref,
    out_ref, spill_ref,
    named_leaves, points, pool, slots, outs, fields, basis_out, features, targets, staged, coeffs, gathered,
    basis, leaf_t, mid_t, base_t, top_t, wide, products, partial, core_got,
    top_coeffs, *rest,
):
    levels = levels_of(devices)
    currents, receives = rest[: len(levels)], rest[len(levels) : 2 * len(levels)]
    (local_sem, spill_sem, fill_sem, out_sem, point_send, point_recv, up_send, down_send, near_recv,
     gather_send, gather_recv, reduce_send, reduce_recv) = rest[2 * len(levels) :]
    count = leaves * M
    part = leaves // CHUNKS
    half = devices // 2
    me = lax.axis_index("leaf")
    core, place = me % 2, me // 2
    has_before, has_after = me > 0, me < devices - 1
    twin = place * 2 + (1 - core)

    own_copy = pltpu.make_async_copy(charges_ref, pool.at[pl.ds(leaves, leaves)], local_sem.at[0])
    own_points = pltpu.make_async_copy(coords_ref, points.at[1], local_sem.at[1])
    near_copy = pltpu.make_async_copy(near_ref, named_leaves, local_sem.at[2])
    own_points.start()
    own_copy.start()
    near_copy.start()

    def digit(stride, size):
        return (place // stride) % size

    def peer(stride, size, turn):
        mine = digit(stride, size)
        other = (mine + turn) % size
        return other, (place + (other - mine) * stride) * 2 + core

    barrier = pltpu.get_barrier_semaphore()
    met = 1
    pl.semaphore_signal(barrier, inc=1, device_id=(twin,), device_id_type=MESH)
    for stride, size in levels:
        for turn in range(1, size):
            met += 1
            pl.semaphore_signal(
                barrier, inc=1, device_id=(peer(stride, size, turn)[1],), device_id_type=MESH
            )

    @pl.when(has_before)
    def _():
        pl.semaphore_signal(barrier, inc=1, device_id=(me - 1,), device_id_type=MESH)

    @pl.when(has_after)
    def _():
        pl.semaphore_signal(barrier, inc=1, device_id=(me + 1,), device_id_type=MESH)

    pl.semaphore_wait(
        barrier, met + jnp.where(has_before, 1, 0) + jnp.where(has_after, 1, 0)
    )

    def remote(src, dst, send, recv, device):
        return pltpu.make_async_remote_copy(
            src_ref=src, dst_ref=dst, send_sem=send, recv_sem=recv,
            device_id=(device,), device_id_type=MESH,
        )

    def points_up():
        return remote(coords_ref, points.at[0], point_send.at[0], point_recv.at[0], me + 1)

    def points_down():
        return remote(coords_ref, points.at[2], point_send.at[1], point_recv.at[1], me - 1)

    def chunk_up(c):
        return remote(
            charges_ref.at[rows(c, part)], pool.at[rows(c, part)],
            up_send.at[c], near_recv.at[0], me + 1,
        )

    def chunk_down(c):
        return remote(
            charges_ref.at[rows(c, part)], pool.at[rows(2 * CHUNKS + c, part)],
            down_send.at[c], near_recv.at[1], me - 1,
        )

    def send_chunk(c):
        @pl.when(has_after)
        def _():
            chunk_up(c).start()

        @pl.when(has_before)
        def _():
            chunk_down(c).start()

    def chunk_left(c):
        @pl.when(has_after)
        def _():
            chunk_up(c).wait_send()

        @pl.when(has_before)
        def _():
            chunk_down(c).wait_send()

    @pl.when(has_after)
    def _():
        points_up().start()

    @pl.when(has_before)
    def _():
        points_down().start()

    @pl.when(jnp.logical_not(has_before))
    def _():
        points[0] = jnp.zeros((3, count), F32)
        pool[:leaves] = jnp.zeros((leaves, M, RHS), BF16)

    @pl.when(jnp.logical_not(has_after))
    def _():
        points[2] = jnp.zeros((3, count), F32)
        pool[2 * leaves :] = jnp.zeros((leaves, M, RHS), BF16)

    send_chunk(0)
    send_chunk(1)

    for p in range(K):
        basis[pl.ds(p, leaves, stride=K), :] = basis_ref[:, p * M : (p + 1) * M].astype(F32)
    basis_out[...] = basis[...].astype(BF16)
    spread(leaf_t, leaf_t_ref, leaves)
    spread(mid_t, mid_t_ref, leaves // 8)
    spread(base_t, base_t_ref, 1)

    own_copy.wait()

    def up_group(i, carry):
        for j in range(8):
            leaf = i * 8 + j
            coeffs[rows(leaf, K), :] = dot(
                basis_out[rows(leaf, K), :], pool[leaves + leaf]
            ).astype(BF16)
        return carry

    lax.fori_loop(0, leaves // 8, up_group, 0)
    mids = []
    for m in range(leaves // 8):
        area = slice(m * 8 * K, (m + 1) * 8 * K)
        mids.append(folded(dot_ta(leaf_t[area, :].astype(BF16), coeffs[area, :])).astype(BF16))
    base = folded(dot_ta(mid_t[...].astype(BF16), jnp.concatenate(mids, axis=0))).astype(BF16)
    spot = core * half + place
    gathered[spot] = jnp.concatenate(
        [base, folded(dot_ta(base_t[...].astype(BF16), base)).astype(BF16)], axis=0
    )

    def featured(which):
        def chunk(i, carry):
            first = pl.multiple_of(i * WIDTH, WIDTH)
            x = (points[which, :, pl.ds(first, WIDTH)] - 0.5) * scale
            h, m = halves(x)
            x = h + m
            norm = x[0:1] * x[0:1] + x[1:2] * x[1:2] + x[2:3] * x[2:3]
            ones = jnp.ones((3, WIDTH), F32)
            zeros = jnp.zeros((FEATURES - 18, WIDTH), F32)
            if which == 1:
                n = pieces(norm + DELTA_SQ * scale * scale)
                write_features(targets, first, WIDTH, [h, h, m, m, *n, ones, zeros])
            n = pieces(norm)
            h, m = -2.0 * h, -2.0 * m
            write_features(staged, 0, WIDTH, [h, m, h, m, ones, *n, zeros])
            for k in range(WIDTH // M):
                features[which * leaves + i * (WIDTH // M) + k] = staged[
                    :, k * M : (k + 1) * M
                ].astype(BF16)
            return carry

        lax.fori_loop(0, count // WIDTH, chunk, 0)

    def gather_copies(level):
        if level == len(levels):
            where = rows(core, half)
            return [remote(
                gathered.at[where], gathered.at[where],
                gather_send.at[level, 0], gather_recv.at[level, 0], twin,
            )]
        stride, size = levels[level]
        copies = []
        for turn in range(1, size):
            where = rows((core * half + place) // stride, stride)
            copies.append(remote(
                gathered.at[where], gathered.at[where],
                gather_send.at[level, turn - 1], gather_recv.at[level, turn - 1],
                peer(stride, size, turn)[1],
            ))
        return copies

    def reduce_copies(level):
        if level == len(levels):
            return [remote(
                partial.at[rows(1 - core, half * 2 * K), :], core_got,
                reduce_send.at[level, 0], reduce_recv.at[level, 0], twin,
            )]
        stride, size = levels[level]
        copies = []
        for turn in range(1, size):
            other, device = peer(stride, size, turn)
            copies.append(remote(
                currents[level].at[rows(other, stride * 2 * K), :], receives[level].at[turn - 1],
                reduce_send.at[level, turn - 1], reduce_recv.at[level, turn - 1], device,
            ))
        return copies

    def start(copies):
        for copy in copies:
            copy.start()

    def arrived(copies):
        for copy in copies:
            copy.wait_recv()

    def sent(copies):
        for copy in copies:
            copy.wait_send()

    def spot_of(device):
        return (device % 2) * half + device // 2

    def couple():
        for t in range(devices // 8):
            total = jnp.zeros((K, RHS), F32)
            for j in range(8):
                total = total + gathered[spot_of(t * 8 + j), K:, :].astype(F32)
            top_coeffs[t] = total.astype(BF16)

        for d in range(devices):
            wide[d] = tiled(gathered[d, :K, :])

        def group(i, carry):
            for j in range(step):
                b = i * step + j
                source = source_ref[b]
                where = (source & 1) * half + (source >> 1)
                products[rows(b, K), :] = dot(
                    products[rows(b, K), :].astype(BF16), wide[where]
                )
            return carry

        lax.fori_loop(0, blocks // step, group, 0)
        named_spot = target_ref[...]
        named_spot = (named_spot & 1) * half + (named_spot >> 1)
        ids = lax.broadcasted_iota(jnp.int32, (devices, blocks), 0)
        chosen = jnp.where(ids == named_spot, 1.0, 0.0).astype(BF16)

        def scatter(i, carry):
            for j in range(8):
                k = i * 8 + j
                terms = products[pl.ds(k, blocks, stride=K), :].astype(BF16)
                partial[pl.ds(k, devices, stride=2 * K), :] = dot(chosen, terms)
            return carry

        lax.fori_loop(0, K // 8, scatter, 0)
        terms = [
            dot(top_t[b * K : (b + 1) * K, :].astype(BF16), tiled(top_coeffs[top_source_ref[b]]))
            for b in range(top_blocks)
        ]
        for t in range(devices // 8):
            total = jnp.zeros((K, RHS), F32)
            for b in range(top_blocks):
                total = total + jnp.where(top_target_ref[b] == t, 1.0, 0.0) * terms[b]
            for j in range(8):
                first = spot_of(t * 8 + j) * 2 * K + K
                partial[first : first + K, :] = total

    def reduced_core():
        mine = partial[rows(core, half * 2 * K), :]
        currents[-1][...] = (mine + core_got[...]).astype(BF16)

    def reduced(level):
        stride, size = levels[level]
        total = currents[level][rows(digit(stride, size), stride * 2 * K), :].astype(F32)
        for turn in range(1, size):
            total = total + receives[level][turn - 1].astype(F32)
        return total

    own_points.wait()
    near_copy.wait()
    featured(1)
    start(gather_copies(0))
    spread(products, blocks_ref, blocks)
    spread(top_t, top_blocks_ref, top_blocks)
    send_chunk(2)

    @pl.when(has_before)
    def _():
        points_up().wait_recv()

    @pl.when(has_after)
    def _():
        points_down().wait_recv()

    featured(0)
    featured(2)
    send_chunk(3)

    stages = []
    for level in range(len(levels)):
        def gather(level=level):
            arrived(gather_copies(level))
            start(gather_copies(level + 1))
        stages.append((2 * level + 1, gather))
    at = 2 * len(levels) + 1

    def coupled():
        arrived(gather_copies(len(levels)))
        couple()

    def core_reduced():
        arrived(reduce_copies(len(levels)))
        reduced_core()

    stages.append((at, coupled))
    stages.append((at + 1, lambda: start(reduce_copies(len(levels)))))
    stages.append((at + 2, core_reduced))
    at += 3
    gap = 2 if len(levels) == 2 else 1
    for level in range(len(levels) - 1, -1, -1):
        stages.append((at, lambda level=level: start(reduce_copies(level))))
        if level:
            def reduce(level=level):
                arrived(reduce_copies(level))
                currents[level - 1][...] = reduced(level).astype(BF16)
            stages.append((at + gap, reduce))
        at += gap + 1

    steps, kept = leaves // EACH, KEEP // EACH
    spilled = steps - kept

    def spill_copy(i):
        return pltpu.make_async_copy(
            slots.at[rows(i, EACH)], spill_ref.at[rows(i, EACH)], spill_sem.at[i]
        )

    def fill_copy(i):
        return pltpu.make_async_copy(
            spill_ref.at[rows(i, EACH)], slots.at[rows(i, EACH)], fill_sem.at[i]
        )

    def out_copy(step, slot):
        return pltpu.make_async_copy(
            outs.at[slot], out_ref.at[rows(step, EACH * M), :], out_sem.at[slot]
        )

    def make(i, carry):
        for when, stage in stages:
            pl.when(i == when)(stage)

        @pl.when(i < CHUNKS - 4)
        def _():
            chunk_left(i + 1)
            send_chunk(i + 4)

        @pl.when(i >= kept)
        def _():
            spill_copy(i - kept).wait()

        for k in range(EACH):
            leaf = i * EACH + k
            mine = targets[:, rows(leaf, M)].T.astype(BF16)
            theirs = jnp.concatenate(
                [features[named_leaves[j, leaf]] for j in range(named)], axis=1
            )
            slots[(i % kept) * EACH + k] = lax.rsqrt(dot(mine, theirs).astype(BF16))

        @pl.when(i < spilled)
        def _():
            spill_copy(i).start()

        return carry

    lax.fori_loop(0, steps, make, 0)
    arrived(reduce_copies(0))
    total = reduced(0)
    base = (
        total[:K] + dot(base_t[...].astype(BF16), tiled(total[K:].astype(BF16)))
    ).astype(BF16)
    mid = dot(mid_t[...].astype(BF16), tiled(base)).astype(BF16)
    for m in range(leaves // 8):
        area = slice(m * 8 * K, (m + 1) * 8 * K)
        fields[area, :] = dot(
            leaf_t[area, :].astype(BF16), tiled(mid[m * K : (m + 1) * K, :])
        ).astype(BF16)

    @pl.when(has_after)
    def _():
        remote(
            charges_ref, pool.at[pl.ds(2 * leaves, leaves)], up_send.at[0], near_recv.at[1], me + 1
        ).wait_recv()

    @pl.when(has_before)
    def _():
        remote(
            charges_ref, pool.at[pl.ds(0, leaves)], up_send.at[0], near_recv.at[0], me - 1
        ).wait_recv()

    def use(i, carry):
        block = jnp.where(i < spilled, i + kept, jnp.where(i < kept, i, i - kept))
        slot = i % 2

        @pl.when(i >= kept)
        def _():
            fill_copy(i - kept).wait()

        @pl.when(i >= 2)
        def _():
            out_copy(i, slot).wait()

        for k in range(EACH):
            leaf = block * EACH + k
            near = jnp.concatenate(
                [pool[named_leaves[j, leaf]] for j in range(named)], axis=0
            )
            total = dot(slots[(i % kept) * EACH + k], near)
            total = total + dot_ta(basis_out[rows(leaf, K), :], fields[rows(leaf, K), :])
            outs[slot, k * M : (k + 1) * M, :] = total.astype(BF16)
        out_copy(block, slot).start()

        @pl.when(i < spilled)
        def _():
            fill_copy(i).start()

        return carry

    lax.fori_loop(0, steps, use, 0)
    out_copy(0, 0).wait()
    out_copy(1, 1).wait()

    for level in range(len(levels) + 1):
        sent(gather_copies(level))
        sent(reduce_copies(level))

    for c in (0, CHUNKS - 3, CHUNKS - 2, CHUNKS - 1):
        chunk_left(c)

    @pl.when(has_after)
    def _():
        points_up().wait_send()

    @pl.when(has_before)
    def _():
        points_down().wait_send()


def per_device(
    coords,
    charges,
    near_leaves,
    leaf_basis,
    leaf_transfer,
    mid_transfer,
    base_transfer,
    base_coupling,
    base_target,
    base_source,
    top_coupling,
    top_target,
    top_source,
):
    leaves, named = near_leaves.shape
    devices = lax.axis_size("leaf")
    blocks, top_blocks = base_coupling.shape[0], top_coupling.shape[0]
    scale = math.sqrt(named * M)
    count = leaves * M
    half = devices // 2
    levels = levels_of(devices)
    widest = max(size for _, size in levels)
    step = max(s for s in range(1, 33) if blocks % s == 0)
    out, _ = pl.pallas_call(
        functools.partial(
            exchange_kernel, devices, leaves, named, blocks, top_blocks, step, scale
        ),
        out_shape=[
            jax.ShapeDtypeStruct((count, RHS), BF16),
            jax.ShapeDtypeStruct((leaves - KEEP, M, named * M), BF16),
        ],
        in_specs=[SMEM] * 3 + [ANY] * 3 + [VMEM] * 7,
        out_specs=[ANY] * 2,
        scratch_shapes=[
            pltpu.SMEM((named, leaves), jnp.int32),
            pltpu.VMEM((3, 3, count), F32),
            pltpu.VMEM((3 * leaves, M, RHS), BF16),
            pltpu.VMEM((KEEP, M, named * M), BF16),
            pltpu.VMEM((2, EACH * M, RHS), BF16),
            pltpu.VMEM((leaves * K, RHS), BF16),
            pltpu.VMEM((leaves * K, M), BF16),
            pltpu.VMEM((3 * leaves, FEATURES, M), BF16),
            pltpu.VMEM((FEATURES, count), F32),
            pltpu.VMEM((FEATURES, WIDTH), F32),
            pltpu.VMEM((leaves * K, RHS), BF16),
            pltpu.VMEM((devices, 2 * K, RHS), BF16),
            pltpu.VMEM((leaves * K, M), F32),
            pltpu.VMEM((leaves * K, LANES), F32),
            pltpu.VMEM((leaves // 8 * K, LANES), F32),
            pltpu.VMEM((K, LANES), F32),
            pltpu.VMEM((top_blocks * K, LANES), F32),
            pltpu.VMEM((devices, LANES, RHS), BF16),
            pltpu.VMEM((blocks * K, RHS), F32),
            pltpu.VMEM((devices * 2 * K, RHS), F32),
            pltpu.VMEM((half * 2 * K, RHS), F32),
            pltpu.VMEM((devices // 8, K, RHS), BF16),
        ]
        + [pltpu.VMEM((stride * size * 2 * K, RHS), BF16) for stride, size in levels]
        + [pltpu.VMEM((size - 1, stride * 2 * K, RHS), BF16) for stride, size in levels]
        + [
            pltpu.SemaphoreType.DMA((3,)),
            pltpu.SemaphoreType.DMA(((leaves - KEEP) // EACH,)),
            pltpu.SemaphoreType.DMA(((leaves - KEEP) // EACH,)),
            pltpu.SemaphoreType.DMA((2,)),
            pltpu.SemaphoreType.DMA((2,)),
            pltpu.SemaphoreType.DMA((2,)),
            pltpu.SemaphoreType.DMA((CHUNKS,)),
            pltpu.SemaphoreType.DMA((CHUNKS,)),
            pltpu.SemaphoreType.DMA((2,)),
        ]
        + [pltpu.SemaphoreType.DMA((len(levels) + 1, widest - 1))] * 4,
        compiler_params=pltpu.CompilerParams(
            vmem_limit_bytes=63 * 1024 * 1024, collective_id=0, has_side_effects=True
        ),
        cost_estimate=pl.CostEstimate(
            flops=16_000_000_000, bytes_accessed=70_000_000, transcendentals=28_000_000
        ),
        name="exchange",
    )(
        base_source, top_target, top_source, near_leaves.T, coords,
        charges.reshape(leaves, M, RHS),
        base_target.T, leaf_basis, leaf_transfer, mid_transfer, base_transfer,
        base_coupling, top_coupling,
    )
    return out


def solution(mesh):
    split, flat = P("leaf", None), P("leaf")
    in_specs = (P(None, "leaf"),) + (split,) * 8 + (flat, split, flat, flat)
    return jax.shard_map(
        per_device, mesh=mesh, in_specs=in_specs, out_specs=split, check_vma=False
    )
```

```python
import functools
import math

import jax
import jax.numpy as jnp
from jax import lax
from jax.experimental import pallas as pl
from jax.experimental.pallas import tpu as pltpu
from jax.sharding import PartitionSpec as P

K = 32
RHS = 128
M = 128
FEATURES = 32
DELTA_SQ = 0.0025
CHUNKS = 16
EACH = 4
KEEP = 36
WIDTH = 2048
LANES = 128
FOLD = LANES // K

F32 = jnp.float32
BF16 = jnp.bfloat16
MESH = pl.DeviceIdType.MESH
VMEM = pl.BlockSpec(memory_space=pltpu.VMEM)
SMEM = pl.BlockSpec(memory_space=pltpu.SMEM)
ANY = pl.BlockSpec(memory_space=pl.ANY)


def dot(a, b):
    return jnp.dot(a, b, preferred_element_type=F32)


def dot_ta(a, b):
    return lax.dot_general(a, b, (((0,), (0,)), ((), ())), preferred_element_type=F32)


def rows(index, size):
    return pl.ds(pl.multiple_of(index * size, size), size)


def halves(x):
    high = x.astype(BF16).astype(F32)
    return high, (x - high).astype(BF16).astype(F32)


def spread(dst, src, count):
    lane = lax.broadcasted_iota(jnp.int32, (1, LANES), 1) // K
    masks = [jnp.where(lane == f, 1.0, 0.0) for f in range(FOLD)]
    for tile in range(K // FOLD):
        slab = src[:, tile * LANES : (tile + 1) * LANES].astype(F32)
        for f in range(FOLD):
            dst[pl.ds(tile * FOLD + f, count, stride=K), :] = slab * masks[f]


def folded(x):
    return sum(x[f * K : (f + 1) * K, :] for f in range(1, FOLD)) + x[:K, :]


def tiled(x):
    return jnp.concatenate([x] * FOLD, axis=0)


def pieces(x):
    high = x.astype(BF16).astype(F32)
    rest = x - high
    middle = rest.astype(BF16).astype(F32)
    return high, middle, (rest - middle).astype(BF16).astype(F32)


def write_features(rows_ref, first, width, parts):
    at = 0
    for part in parts:
        rows_ref[at : at + part.shape[0], pl.ds(first, width)] = part
        at += part.shape[0]


def groups_of(named):
    return [range(j, min(j + 2, named)) for j in range(0, named, 2)]


def levels_of(devices):
    plane = devices // 8
    if plane <= 4:
        return [(1, plane), (plane, 4)]
    low = 2 ** (int(math.log2(plane)) // 2)
    return [(1, low), (low, plane // low), (plane, 4)]


def exchange_kernel(
    devices, leaves, named, blocks, top_blocks, step, scale,
    source_ref, top_target_ref, top_source_ref,
    near_ref, coords_ref, charges_ref,
    target_ref, basis_ref, leaf_t_ref, mid_t_ref, base_t_ref, blocks_ref, top_blocks_ref,
    out_ref, spill_ref,
    named_leaves, points, pool, slots, outs, fields, basis_out, features, targets, staged, coeffs, gathered,
    basis, leaf_t, mid_t, base_t, top_t, wide, products, partial, core_got,
    top_coeffs, *rest,
):
    levels = levels_of(devices)
    currents, receives = rest[: len(levels)], rest[len(levels) : 2 * len(levels)]
    (local_sem, spill_sem, fill_sem, out_sem, point_send, point_recv, up_send, down_send, near_recv,
     gather_send, gather_recv, reduce_send, reduce_recv) = rest[2 * len(levels) :]
    count = leaves * M
    part = leaves // CHUNKS
    half = devices // 2
    me = lax.axis_index("leaf")
    core, place = me % 2, me // 2
    has_before, has_after = me > 0, me < devices - 1
    twin = place * 2 + (1 - core)

    own_copy = pltpu.make_async_copy(charges_ref, pool.at[pl.ds(leaves, leaves)], local_sem.at[0])
    own_points = pltpu.make_async_copy(coords_ref, points.at[1], local_sem.at[1])
    near_copy = pltpu.make_async_copy(near_ref, named_leaves, local_sem.at[2])
    own_points.start()
    own_copy.start()
    near_copy.start()

    def digit(stride, size):
        return (place // stride) % size

    def peer(stride, size, turn):
        mine = digit(stride, size)
        other = (mine + turn) % size
        return other, (place + (other - mine) * stride) * 2 + core

    barrier = pltpu.get_barrier_semaphore()
    met = 1
    pl.semaphore_signal(barrier, inc=1, device_id=(twin,), device_id_type=MESH)
    for stride, size in levels:
        for turn in range(1, size):
            met += 1
            pl.semaphore_signal(
                barrier, inc=1, device_id=(peer(stride, size, turn)[1],), device_id_type=MESH
            )

    @pl.when(has_before)
    def _():
        pl.semaphore_signal(barrier, inc=1, device_id=(me - 1,), device_id_type=MESH)

    @pl.when(has_after)
    def _():
        pl.semaphore_signal(barrier, inc=1, device_id=(me + 1,), device_id_type=MESH)

    pl.semaphore_wait(
        barrier, met + jnp.where(has_before, 1, 0) + jnp.where(has_after, 1, 0)
    )

    def remote(src, dst, send, recv, device):
        return pltpu.make_async_remote_copy(
            src_ref=src, dst_ref=dst, send_sem=send, recv_sem=recv,
            device_id=(device,), device_id_type=MESH,
        )

    def points_up():
        return remote(coords_ref, points.at[0], point_send.at[0], point_recv.at[0], me + 1)

    def points_down():
        return remote(coords_ref, points.at[2], point_send.at[1], point_recv.at[1], me - 1)

    def chunk_up(c):
        return remote(
            charges_ref.at[rows(c, part)], pool.at[rows(c, part)],
            up_send.at[c], near_recv.at[0], me + 1,
        )

    def chunk_down(c):
        return remote(
            charges_ref.at[rows(c, part)], pool.at[rows(2 * CHUNKS + c, part)],
            down_send.at[c], near_recv.at[1], me - 1,
        )

    def send_chunk(c):
        @pl.when(has_after)
        def _():
            chunk_up(c).start()

        @pl.when(has_before)
        def _():
            chunk_down(c).start()

    def chunk_left(c):
        @pl.when(has_after)
        def _():
            chunk_up(c).wait_send()

        @pl.when(has_before)
        def _():
            chunk_down(c).wait_send()

    @pl.when(has_after)
    def _():
        points_up().start()

    @pl.when(has_before)
    def _():
        points_down().start()

    @pl.when(jnp.logical_not(has_before))
    def _():
        points[0] = jnp.zeros((3, count), F32)
        pool[:leaves] = jnp.zeros((leaves, M, RHS), BF16)

    @pl.when(jnp.logical_not(has_after))
    def _():
        points[2] = jnp.zeros((3, count), F32)
        pool[2 * leaves :] = jnp.zeros((leaves, M, RHS), BF16)

    send_chunk(0)
    send_chunk(1)

    for p in range(K):
        basis[pl.ds(p, leaves, stride=K), :] = basis_ref[:, p * M : (p + 1) * M].astype(F32)
    basis_out[...] = basis[...].astype(BF16)
    spread(leaf_t, leaf_t_ref, leaves)
    spread(mid_t, mid_t_ref, leaves // 8)
    spread(base_t, base_t_ref, 1)

    own_copy.wait()

    def up_group(i, carry):
        for j in range(8):
            leaf = i * 8 + j
            coeffs[rows(leaf, K), :] = dot(
                basis_out[rows(leaf, K), :], pool[leaves + leaf]
            ).astype(BF16)
        return carry

    lax.fori_loop(0, leaves // 8, up_group, 0)
    mids = []
    for m in range(leaves // 8):
        area = slice(m * 8 * K, (m + 1) * 8 * K)
        mids.append(folded(dot_ta(leaf_t[area, :].astype(BF16), coeffs[area, :])).astype(BF16))
    base = folded(dot_ta(mid_t[...].astype(BF16), jnp.concatenate(mids, axis=0))).astype(BF16)
    spot = core * half + place
    gathered[spot] = jnp.concatenate(
        [base, folded(dot_ta(base_t[...].astype(BF16), base)).astype(BF16)], axis=0
    )

    def featured(which):
        def chunk(i, carry):
            first = pl.multiple_of(i * WIDTH, WIDTH)
            x = (points[which, :, pl.ds(first, WIDTH)] - 0.5) * scale
            h, m = halves(x)
            x = h + m
            norm = x[0:1] * x[0:1] + x[1:2] * x[1:2] + x[2:3] * x[2:3]
            ones = jnp.ones((3, WIDTH), F32)
            zeros = jnp.zeros((FEATURES - 18, WIDTH), F32)
            if which == 1:
                n = pieces(norm + DELTA_SQ * scale * scale)
                write_features(targets, first, WIDTH, [h, h, m, m, *n, ones, zeros])
            n = pieces(norm)
            h, m = -2.0 * h, -2.0 * m
            write_features(staged, 0, WIDTH, [h, m, h, m, ones, *n, zeros])
            for k in range(WIDTH // M):
                features[which * leaves + i * (WIDTH // M) + k] = staged[
                    :, k * M : (k + 1) * M
                ].astype(BF16)
            return carry

        lax.fori_loop(0, count // WIDTH, chunk, 0)

    def gather_copies(level):
        if level == len(levels):
            where = rows(core, half)
            return [remote(
                gathered.at[where], gathered.at[where],
                gather_send.at[level, 0], gather_recv.at[level, 0], twin,
            )]
        stride, size = levels[level]
        copies = []
        for turn in range(1, size):
            where = rows((core * half + place) // stride, stride)
            copies.append(remote(
                gathered.at[where], gathered.at[where],
                gather_send.at[level, turn - 1], gather_recv.at[level, turn - 1],
                peer(stride, size, turn)[1],
            ))
        return copies

    def reduce_copies(level):
        if level == len(levels):
            return [remote(
                partial.at[rows(1 - core, half * 2 * K), :], core_got,
                reduce_send.at[level, 0], reduce_recv.at[level, 0], twin,
            )]
        stride, size = levels[level]
        copies = []
        for turn in range(1, size):
            other, device = peer(stride, size, turn)
            copies.append(remote(
                currents[level].at[rows(other, stride * 2 * K), :], receives[level].at[turn - 1],
                reduce_send.at[level, turn - 1], reduce_recv.at[level, turn - 1], device,
            ))
        return copies

    def start(copies):
        for copy in copies:
            copy.start()

    def arrived(copies):
        for copy in copies:
            copy.wait_recv()

    def sent(copies):
        for copy in copies:
            copy.wait_send()

    def spot_of(device):
        return (device % 2) * half + device // 2

    def couple():
        for t in range(devices // 8):
            total = jnp.zeros((K, RHS), F32)
            for j in range(8):
                total = total + gathered[spot_of(t * 8 + j), K:, :].astype(F32)
            top_coeffs[t] = total.astype(BF16)

        for d in range(devices):
            wide[d] = tiled(gathered[d, :K, :])

        def group(i, carry):
            for j in range(step):
                b = i * step + j
                source = source_ref[b]
                where = (source & 1) * half + (source >> 1)
                products[rows(b, K), :] = dot(
                    products[rows(b, K), :].astype(BF16), wide[where]
                )
            return carry

        lax.fori_loop(0, blocks // step, group, 0)
        named_spot = target_ref[...]
        named_spot = (named_spot & 1) * half + (named_spot >> 1)
        ids = lax.broadcasted_iota(jnp.int32, (devices, blocks), 0)
        chosen = jnp.where(ids == named_spot, 1.0, 0.0).astype(BF16)

        def scatter(i, carry):
            for j in range(8):
                k = i * 8 + j
                terms = products[pl.ds(k, blocks, stride=K), :].astype(BF16)
                partial[pl.ds(k, devices, stride=2 * K), :] = dot(chosen, terms)
            return carry

        lax.fori_loop(0, K // 8, scatter, 0)
        terms = [
            dot(top_t[b * K : (b + 1) * K, :].astype(BF16), tiled(top_coeffs[top_source_ref[b]]))
            for b in range(top_blocks)
        ]
        for t in range(devices // 8):
            total = jnp.zeros((K, RHS), F32)
            for b in range(top_blocks):
                total = total + jnp.where(top_target_ref[b] == t, 1.0, 0.0) * terms[b]
            for j in range(8):
                first = spot_of(t * 8 + j) * 2 * K + K
                partial[first : first + K, :] = total

    def reduced_core():
        mine = partial[rows(core, half * 2 * K), :]
        currents[-1][...] = (mine + core_got[...]).astype(BF16)

    def reduced(level):
        stride, size = levels[level]
        total = currents[level][rows(digit(stride, size), stride * 2 * K), :].astype(F32)
        for turn in range(1, size):
            total = total + receives[level][turn - 1].astype(F32)
        return total

    own_points.wait()
    near_copy.wait()
    featured(1)
    start(gather_copies(0))
    spread(products, blocks_ref, blocks)
    spread(top_t, top_blocks_ref, top_blocks)
    send_chunk(2)

    @pl.when(has_before)
    def _():
        points_up().wait_recv()

    @pl.when(has_after)
    def _():
        points_down().wait_recv()

    featured(0)
    featured(2)
    send_chunk(3)

    stages = []
    for level in range(len(levels)):
        def gather(level=level):
            arrived(gather_copies(level))
            start(gather_copies(level + 1))
        stages.append((2 * level, gather))
    at = 2 * len(levels)

    def coupled():
        arrived(gather_copies(len(levels)))
        couple()

    def core_reduced():
        arrived(reduce_copies(len(levels)))
        reduced_core()

    stages.append((at, coupled))
    stages.append((at + 1, lambda: start(reduce_copies(len(levels)))))
    stages.append((at + 2, core_reduced))
    at += 3
    gap = 1
    for level in range(len(levels) - 1, -1, -1):
        stages.append((at, lambda level=level: start(reduce_copies(level))))
        if level:
            def reduce(level=level):
                arrived(reduce_copies(level))
                currents[level - 1][...] = reduced(level).astype(BF16)
            stages.append((at + gap, reduce))
        at += gap + 1

    steps, kept = leaves // EACH, KEEP // EACH
    spilled = steps - kept

    def spill_copy(i):
        return pltpu.make_async_copy(
            slots.at[rows(i, EACH)], spill_ref.at[rows(i, EACH)], spill_sem.at[i]
        )

    def fill_copy(i):
        return pltpu.make_async_copy(
            spill_ref.at[rows(i, EACH)], slots.at[rows(i, EACH)], fill_sem.at[i]
        )

    def out_copy(step, slot):
        return pltpu.make_async_copy(
            outs.at[slot], out_ref.at[rows(step, EACH * M), :], out_sem.at[slot]
        )

    def make(i, carry):
        for when, stage in stages:
            pl.when(i == when)(stage)

        @pl.when(i < CHUNKS - 4)
        def _():
            chunk_left(i + 1)
            send_chunk(i + 4)

        @pl.when(i >= kept)
        def _():
            spill_copy(i - kept).wait()

        for k in range(EACH):
            leaf = i * EACH + k
            mine = targets[:, rows(leaf, M)].T.astype(BF16)
            theirs = jnp.concatenate(
                [features[named_leaves[j, leaf]] for j in range(named)], axis=1
            )
            slots[(i % kept) * EACH + k] = lax.rsqrt(dot(mine, theirs).astype(BF16))

        @pl.when(i < spilled)
        def _():
            spill_copy(i).start()

        return carry

    lax.fori_loop(0, steps, make, 0)
    arrived(reduce_copies(0))
    total = reduced(0)
    base = (
        total[:K] + dot(base_t[...].astype(BF16), tiled(total[K:].astype(BF16)))
    ).astype(BF16)
    mid = dot(mid_t[...].astype(BF16), tiled(base)).astype(BF16)
    for m in range(leaves // 8):
        area = slice(m * 8 * K, (m + 1) * 8 * K)
        fields[area, :] = dot(
            leaf_t[area, :].astype(BF16), tiled(mid[m * K : (m + 1) * K, :])
        ).astype(BF16)

    @pl.when(has_after)
    def _():
        remote(
            charges_ref, pool.at[pl.ds(2 * leaves, leaves)], up_send.at[0], near_recv.at[1], me + 1
        ).wait_recv()

    @pl.when(has_before)
    def _():
        remote(
            charges_ref, pool.at[pl.ds(0, leaves)], up_send.at[0], near_recv.at[0], me - 1
        ).wait_recv()

    def use(i, carry):
        block = jnp.where(i < spilled, i + kept, jnp.where(i < kept, i, i - kept))
        slot = i % 2

        @pl.when(i >= kept)
        def _():
            fill_copy(i - kept).wait()

        @pl.when(i >= 2)
        def _():
            out_copy(i, slot).wait()

        for k in range(EACH):
            leaf = block * EACH + k
            near = jnp.concatenate(
                [pool[named_leaves[j, leaf]] for j in range(named)], axis=0
            )
            total = dot(slots[(i % kept) * EACH + k], near)
            total = total + dot_ta(basis_out[rows(leaf, K), :], fields[rows(leaf, K), :])
            outs[slot, k * M : (k + 1) * M, :] = total.astype(BF16)
        out_copy(block, slot).start()

        @pl.when(i < spilled)
        def _():
            fill_copy(i).start()

        return carry

    lax.fori_loop(0, steps, use, 0)
    out_copy(0, 0).wait()
    out_copy(1, 1).wait()

    for level in range(len(levels) + 1):
        sent(gather_copies(level))
        sent(reduce_copies(level))

    for c in (0, CHUNKS - 3, CHUNKS - 2, CHUNKS - 1):
        chunk_left(c)

    @pl.when(has_after)
    def _():
        points_up().wait_send()

    @pl.when(has_before)
    def _():
        points_down().wait_send()


def per_device(
    coords,
    charges,
    near_leaves,
    leaf_basis,
    leaf_transfer,
    mid_transfer,
    base_transfer,
    base_coupling,
    base_target,
    base_source,
    top_coupling,
    top_target,
    top_source,
):
    leaves, named = near_leaves.shape
    devices = lax.axis_size("leaf")
    blocks, top_blocks = base_coupling.shape[0], top_coupling.shape[0]
    scale = math.sqrt(named * M)
    count = leaves * M
    half = devices // 2
    levels = levels_of(devices)
    widest = max(size for _, size in levels)
    step = max(s for s in range(1, 33) if blocks % s == 0)
    out, _ = pl.pallas_call(
        functools.partial(
            exchange_kernel, devices, leaves, named, blocks, top_blocks, step, scale
        ),
        out_shape=[
            jax.ShapeDtypeStruct((count, RHS), BF16),
            jax.ShapeDtypeStruct((leaves - KEEP, M, named * M), BF16),
        ],
        in_specs=[SMEM] * 3 + [ANY] * 3 + [VMEM] * 7,
        out_specs=[ANY] * 2,
        scratch_shapes=[
            pltpu.SMEM((named, leaves), jnp.int32),
            pltpu.VMEM((3, 3, count), F32),
            pltpu.VMEM((3 * leaves, M, RHS), BF16),
            pltpu.VMEM((KEEP, M, named * M), BF16),
            pltpu.VMEM((2, EACH * M, RHS), BF16),
            pltpu.VMEM((leaves * K, RHS), BF16),
            pltpu.VMEM((leaves * K, M), BF16),
            pltpu.VMEM((3 * leaves, FEATURES, M), BF16),
            pltpu.VMEM((FEATURES, count), F32),
            pltpu.VMEM((FEATURES, WIDTH), F32),
            pltpu.VMEM((leaves * K, RHS), BF16),
            pltpu.VMEM((devices, 2 * K, RHS), BF16),
            pltpu.VMEM((leaves * K, M), F32),
            pltpu.VMEM((leaves * K, LANES), F32),
            pltpu.VMEM((leaves // 8 * K, LANES), F32),
            pltpu.VMEM((K, LANES), F32),
            pltpu.VMEM((top_blocks * K, LANES), F32),
            pltpu.VMEM((devices, LANES, RHS), BF16),
            pltpu.VMEM((blocks * K, RHS), F32),
            pltpu.VMEM((devices * 2 * K, RHS), F32),
            pltpu.VMEM((half * 2 * K, RHS), F32),
            pltpu.VMEM((devices // 8, K, RHS), BF16),
        ]
        + [pltpu.VMEM((stride * size * 2 * K, RHS), BF16) for stride, size in levels]
        + [pltpu.VMEM((size - 1, stride * 2 * K, RHS), BF16) for stride, size in levels]
        + [
            pltpu.SemaphoreType.DMA((3,)),
            pltpu.SemaphoreType.DMA(((leaves - KEEP) // EACH,)),
            pltpu.SemaphoreType.DMA(((leaves - KEEP) // EACH,)),
            pltpu.SemaphoreType.DMA((2,)),
            pltpu.SemaphoreType.DMA((2,)),
            pltpu.SemaphoreType.DMA((2,)),
            pltpu.SemaphoreType.DMA((CHUNKS,)),
            pltpu.SemaphoreType.DMA((CHUNKS,)),
            pltpu.SemaphoreType.DMA((2,)),
        ]
        + [pltpu.SemaphoreType.DMA((len(levels) + 1, widest - 1))] * 4,
        compiler_params=pltpu.CompilerParams(
            vmem_limit_bytes=63 * 1024 * 1024, collective_id=0, has_side_effects=True
        ),
        cost_estimate=pl.CostEstimate(
            flops=16_000_000_000, bytes_accessed=70_000_000, transcendentals=28_000_000
        ),
        name="exchange",
    )(
        base_source, top_target, top_source, near_leaves.T, coords,
        charges.reshape(leaves, M, RHS),
        base_target.T, leaf_basis, leaf_transfer, mid_transfer, base_transfer,
        base_coupling, top_coupling,
    )
    return out


def solution(mesh):
    split, flat = P("leaf", None), P("leaf")
    in_specs = (P(None, "leaf"),) + (split,) * 8 + (flat, split, flat, flat)
    return jax.shard_map(
        per_device, mesh=mesh, in_specs=in_specs, out_specs=split, check_vma=False
    )
```
